32 devices in a mesh: px: 8 (over z, y), py: 4 (over x, core).
Axes of the slice: x: 2, y: 2, z: 4, core: 2. Of those that a mesh axis runs over, the one named last changes fastest.
Arguments:
- initial_field: float32 [1, 2048, 2048], P(None, ('px', 'py')), may hold values from -6 to 6
- target_field: float32 [1, 2048, 2048], P(None, ('px', 'py')), may hold values from -6 to 6
- forcing: float32 [2, 2048, 2048], P(None, ('px', 'py')), may hold values from -6 to 6
Outputs:
- next_field: float32 [1, 2048, 2048], P(None, ('px', 'py'))
- objective: float32 [], replicated
- field_grad: float32 [1, 2048, 2048], P(None, ('px', 'py'))
- forcing_grad: float32 [2, 2048, 2048], P(None, ('px', 'py'))
The draws below stay inside these ranges and needn't reach their ends.
All inputs are finite; a program needn't handle non-finite values.
Results may differ from the reference program's by a relative error of at most 0.00014.
Values sent between devices are 32-bit elements; how exact they have to be, the bound alone decides.
A program may use at most 128 MiB of HBM per device.

```python
import jax
import jax.numpy as jnp
from jax import lax

NX = 2048
NY = 2048
MEMBERS = 1


def block_scale(own_key, dims, shards, low, largest):
    def one(dim, shards_of):
        heights = jax.random.uniform(jax.random.fold_in(jax.random.fold_in(own_key, 6), dim), (shards_of,), jnp.float32, low / len(shards), largest / len(shards))
        return jnp.repeat(jnp.exp(heights), dims[dim] // shards_of).reshape((-1,) + (1,) * (len(dims) - dim - 1))

    level = one(*shards[0])
    for cut in shards[1:]:
        level = level * one(*cut)
    return level


def gaussian(key, extent, deviation, bound, cuts=(), held_as=jnp.bfloat16):
    values = deviation * jax.random.normal(key, extent, jnp.float32)
    if cuts:
        values = values * block_scale(key, extent, cuts, -0.22, 0.18)
    return jnp.clip(values, -bound, bound).astype(held_as)


def setup_inputs(seed: int = 0) -> dict:
    arg_keys = jax.random.split(jax.random.key(seed), 4)
    initial_field = gaussian(arg_keys[0], (MEMBERS, NX, NY), 1.0, 6.0, ((1, 32),), jnp.float32)
    target_field = gaussian(arg_keys[1], (MEMBERS, NX, NY), 1.0, 6.0, ((1, 32),), jnp.float32)
    forcing = gaussian(arg_keys[2], (2, NY, NX), 1.0, 6.0, ((1, 32),), jnp.float32)
    return {"initial_field": initial_field, "target_field": target_field, "forcing": forcing}


time_step = 0.25

def wavenumbers(count):
    position = jnp.arange(count, dtype=jnp.int32)
    signed = jnp.where(position < count // 2, position, position - count)
    waves = (4.0 * signed.astype(jnp.float32) / count).astype(jnp.float32)
    derive = jnp.where(position == count // 2, jnp.float32(0.0), waves).astype(jnp.float32)
    return (waves, derive)

def advance(field, forcing):
    wave_first, deriv_first = wavenumbers(NX)
    wave_second, deriv_second = wavenumbers(NY)
    wave_square = wave_first[:, None] ** 2 + wave_second[None, :] ** 2
    denominator = 1.0 + time_step * (wave_square * wave_square - wave_square)
    state_hat = jnp.fft.fft2(field, norm='ortho')
    grad_first = jnp.fft.ifft2(1j * deriv_first[:, None] * state_hat, norm='ortho').real
    grad_second = jnp.fft.ifft2(1j * deriv_second[None, :] * state_hat, norm='ortho').real
    nonlinear = -0.5 * (grad_first * grad_first + grad_second * grad_second)
    nonlinear_hat = jnp.fft.fft2(nonlinear, norm='ortho')
    forcing_hat = lax.complex(forcing[0].T, forcing[1].T)
    next_hat = (state_hat + time_step * (nonlinear_hat + forcing_hat)) / denominator
    return jnp.fft.ifft2(next_hat, norm='ortho').real

def reference(initial_field, target_field, forcing):

    def one_member(pair):
        field, goal = pair
        next_one, pullback = jax.vjp(advance, field, forcing)
        residual = next_one - goal
        grad_one, forcing_one = pullback(residual)
        return (next_one, jnp.sum(residual * residual), grad_one, forcing_one)
    next_field, squares, field_grad, forcing_parts = lax.map(one_member, (initial_field, target_field))
    objective = 0.5 * jnp.sum(squares) / (MEMBERS * NX * NY)
    forcing_grad = lax.optimization_barrier(jnp.sum(forcing_parts, axis=0))
    return (next_field, objective, field_grad, forcing_grad)
```

```python
import functools
import math

import jax
import jax.numpy as jnp
import numpy as np
from jax import lax
from jax.experimental import pallas as pl
from jax.experimental.pallas import tpu as pltpu
from jax.sharding import PartitionSpec as P

time_step = 0.25
axes = ("px", "py")
TILE = 128


def split_length(length):
    inner = 256 if length % 256 == 0 else TILE
    return (length // inner, inner)


def small_dft(items, sign):
    count = len(items)
    if count == 1:
        return items
    evens = small_dft(items[0::2], sign)
    odds = small_dft(items[1::2], sign)
    low, high = [], []
    for k in range(count // 2):
        odd_re, odd_im = odds[k]
        if 4 * k == count:
            odd_re, odd_im = (-odd_im, odd_re) if sign > 0 else (odd_im, -odd_re)
        elif k:
            c = math.cos(2.0 * math.pi * k / count)
            s = sign * math.sin(2.0 * math.pi * k / count)
            if abs(abs(c) - abs(s)) < 1e-12:
                sc, ss = math.copysign(1.0, c), math.copysign(1.0, s)
                odd_re, odd_im = (
                    c * (odd_re - sc * ss * odd_im),
                    c * (odd_im + sc * ss * odd_re),
                )
            else:
                odd_re, odd_im = (c * odd_re - s * odd_im, c * odd_im + s * odd_re)
        even_re, even_im = evens[k]
        low.append((even_re + odd_re, even_im + odd_im))
        high.append((even_re - odd_re, even_im - odd_im))
    return low + high


def halves(value):
    top = value.astype(jnp.bfloat16)
    return top, (value - top.astype(jnp.float32)).astype(jnp.bfloat16)


def tables(length):
    outer, inner = split_length(length)
    angle = 2.0 * np.pi * np.outer(np.arange(outer), np.arange(inner)) / length
    twiddle = np.stack([np.cos(angle), np.sin(angle)]) / math.sqrt(length)
    angle = 2.0 * np.pi * (np.outer(np.arange(inner), np.arange(inner)) % inner) / inner
    c, s = np.cos(angle), np.sin(angle)
    both = []
    for sign in (-1.0, 1.0):
        full = np.block([[c, sign * s], [-sign * s, c]])
        top = full.astype(jnp.bfloat16)
        low = (full - top.astype(np.float64)).astype(jnp.bfloat16)
        both.append(np.stack([top, low]))
    return twiddle.astype(np.float32), np.stack(both)


class Pieces:
    def __init__(self, length, rows, twiddle, matrix, turned, top, low, grid_out):
        self.length, self.rows = length, rows
        self.outer, self.inner = split_length(length)
        self.twiddle, self.matrix = twiddle, matrix
        self.turned, self.top, self.low, self.z = turned, top, low, grid_out
        self.step = math.gcd(rows, 16)

    def chunks(self, body):
        def run(i, carry):
            body(pl.multiple_of(i * self.step, self.step))
            return carry

        lax.fori_loop(0, self.rows // self.step, run, 0)

    def put(self, k, at, part, value):
        lanes = pl.ds(part * self.inner, self.inner)
        top, low = halves(value)
        self.top[k, at, lanes] = top
        self.low[k, at, lanes] = low

    def get(self, k, at, part):
        return self.z[k, at, pl.ds(part * self.inner, self.inner)]

    def multiply(self, sign, real_in=False, real_out=False):
        which = 0 if sign < 0 else 1
        deep = self.inner if real_in else 2 * self.inner
        wide = self.inner if real_out else 2 * self.inner
        count = self.outer * self.rows
        top = self.top[:, :, :deep].reshape(count, deep)
        low = self.low[:, :, :deep].reshape(count, deep)
        right_top = self.matrix[which, 0, :deep, :wide]
        right_low = self.matrix[which, 1, :deep, :wide]
        dot = functools.partial(jnp.dot, preferred_element_type=jnp.float32)
        total = dot(top, right_top) + dot(low, right_top) + dot(top, right_low)
        self.z[:, :, :wide] = total.reshape(self.outer, self.rows, wide)

    def twist(self, k, pair, sign):
        c = self.twiddle[0, pl.ds(k, 1), :]
        s = self.twiddle[1, pl.ds(k, 1), :]
        s = s if sign > 0 else -s
        re, im = pair
        return (re * c - im * s, re * s + im * c)

    def incoming(self, source, sign, real_out=False):
        rows, blocks = self.rows, max(TILE // self.rows, 1)
        span = blocks * rows
        for t in range(self.length // span):
            tile = source[pl.ds(t * blocks, blocks), :rows, :].reshape(span, 2 * rows)
            self.turned[: 2 * rows, pl.ds(t * span, span)] = tile.T

        def body(r0):
            items = []
            for j in range(self.outer):
                lanes = pl.ds(j * self.inner, self.inner)
                items.append((
                    self.turned[pl.ds(r0, self.step), lanes],
                    self.turned[pl.ds(rows + r0, self.step), lanes],
                ))
            for k, pair in enumerate(small_dft(items, sign)):
                re, im = self.twist(k, pair, sign)
                self.put(k, pl.ds(r0, self.step), 0, re)
                self.put(k, pl.ds(r0, self.step), 1, im)

        self.chunks(body)
        self.multiply(sign, real_out=real_out)

    def outgoing(self, sign, real_in, result):
        self.multiply(sign, real_in=real_in)
        rows = self.rows

        def body(r0):
            at = pl.ds(r0, self.step)
            items = [
                self.twist(k, (self.get(k, at, 0), self.get(k, at, 1)), sign)
                for k in range(self.outer)
            ]
            for j, (re, im) in enumerate(small_dft(items, sign)):
                for piece in range(self.inner // rows):
                    to = j * (self.inner // rows) + piece
                    lanes = slice(piece * rows, (piece + 1) * rows)
                    result[to, at, pl.ds(0, rows)] = re[:, lanes]
                    result[to, at, pl.ds(rows, rows)] = im[:, lanes]

        self.chunks(body)

    def spread(self, first, second, strided, result):
        rows, fill = self.rows, TILE - 2 * self.rows
        for t in range(self.length // TILE):
            lanes = pl.ds(t * TILE, TILE)
            parts = [first[:, lanes], second[:, lanes]]
            if fill:
                parts.append(jnp.zeros((fill, TILE), jnp.float32))
            strided[pl.ds(t * TILE, TILE), :] = jnp.concatenate(parts, axis=0).T
        for k in range(self.outer):
            slab = strided[pl.ds(k, self.inner, stride=self.outer), :].T
            result[k] = slab[: 2 * rows, :]

    def collect(self, slabs, strided, results):
        rows = self.rows
        for k in range(self.outer):
            slab = slabs(k)
            fill = TILE - slab.shape[0]
            if fill:
                slab = jnp.concatenate([slab, jnp.zeros((fill, self.inner), jnp.float32)], axis=0)
            strided[pl.ds(k, self.inner, stride=self.outer), :] = slab.T
        for t in range(self.length // TILE):
            block = strided[pl.ds(t * TILE, TILE), :].T
            for i, result in enumerate(results):
                result[:, pl.ds(t * TILE, TILE)] = block[i * rows : (i + 1) * rows, :]


def signed_waves(position, count):
    signed = jnp.where(position < count // 2, position, position - count)
    waves = 4.0 * signed.astype(jnp.float32) / count
    return waves, jnp.where(position == count // 2, jnp.float32(0.0), waves)


def wave_grids(piece, device, r0, k):
    shape = (piece.step, piece.inner)
    first = piece.outer * lax.broadcasted_iota(jnp.int32, (1, piece.inner), 1) + k
    second = device * piece.rows + r0 + lax.broadcasted_iota(jnp.int32, shape, 0)
    wave_first, deriv_first = signed_waves(first, piece.length)
    wave_second, deriv_second = signed_waves(second, piece.length)
    square = wave_first * wave_first + wave_second * wave_second
    denominator = 1.0 + time_step * (square * square - square)
    return deriv_first, deriv_second, denominator


def start_kernel(length, rows, field, target, twiddle, matrix, out, target_p, turned, top, low, z, strided):
    piece = Pieces(length, rows, twiddle, matrix, turned, top, low, z)
    piece.spread(field, target, strided, target_p)

    def body(r0):
        for k in range(piece.outer):
            piece.put(k, pl.ds(r0, piece.step), 0, target_p[k, pl.ds(r0, piece.step), :])

    piece.chunks(body)
    piece.outgoing(-1.0, True, out)


def spread_kernel(length, rows, forcing, result, strided):
    piece = Pieces(length, rows, None, None, None, None, None, None)
    piece.spread(forcing.at[0], forcing.at[1], strided, result)


def collect_kernel(length, rows, slabs, result, strided):
    piece = Pieces(length, rows, None, None, None, None, None, None)
    piece.collect(lambda k: slabs[k], strided, [result.at[i] for i in range(result.shape[0])])


def spectral_kernel(kind, length, rows, *refs):
    device_ref, source, *rest = refs
    device = device_ref[0]
    if kind == "slope":
        twiddle, matrix, out, state_out, *scratch = rest
    elif kind == "next":
        state_in, forcing_in, twiddle, matrix, out, *scratch = rest
    elif kind == "misfit":
        twiddle, matrix, out, coef_out, total_out, *scratch = rest
    else:
        coef_in, twiddle, matrix, out, *scratch = rest
    piece = Pieces(length, rows, twiddle, matrix, *scratch[:4])
    piece.incoming(source, -1.0)

    def body(r0):
        at = pl.ds(r0, piece.step)
        also = pl.ds(rows + r0, piece.step)
        for k in range(piece.outer):
            re, im = piece.get(k, at, 0), piece.get(k, at, 1)
            deriv_first, deriv_second, denominator = wave_grids(piece, device, r0, k)
            if kind == "slope":
                state_out[k, at, :], state_out[k, also, :] = re, im
                new_re = -deriv_first * im - deriv_second * re
                new_im = deriv_first * re - deriv_second * im
            elif kind == "next":
                inverse = 1.0 / denominator
                new_re = (state_in[k, at, :] + time_step * (re + forcing_in[k, at, :])) * inverse
                new_im = (state_in[k, also, :] + time_step * (im + forcing_in[k, also, :])) * inverse
            elif kind == "misfit":
                inverse = 1.0 / denominator
                new_re, new_im = time_step * (re * inverse), time_step * (im * inverse)
                coef_out[k, at, :], coef_out[k, also, :] = new_re, new_im
            else:
                scale = 1.0 / time_step
                new_re = scale * coef_in[k, at, :] - deriv_first * im + deriv_second * re
                new_im = scale * coef_in[k, also, :] + deriv_first * re + deriv_second * im
            piece.put(k, at, 0, new_re)
            piece.put(k, at, 1, new_im)

    piece.chunks(body)
    piece.outgoing(1.0, False, out)
    if kind == "misfit":
        total_out[...] = jnp.sum(source[:, pl.ds(rows, 8), :], axis=0)


def physical_kernel(kind, length, rows, *refs):
    source, *rest = refs
    if kind == "nonlinear":
        twiddle, matrix, out, grads_out, *scratch = rest
    elif kind == "residual":
        target_p, twiddle, matrix, out, field_out, *scratch = rest
    elif kind == "joint":
        grads_in, twiddle, matrix, out, *scratch = rest
    else:
        twiddle, matrix, field_out, *scratch = rest
    piece = Pieces(length, rows, twiddle, matrix, *scratch[:4])
    piece.incoming(source, 1.0, real_out=kind != "nonlinear")
    if kind in ("residual", "last"):
        piece.collect(lambda k: piece.get(k, pl.ds(0, rows), 0), scratch[4], [field_out])
    if kind == "last":
        return
    if kind == "residual":
        total = scratch[5]
        total[...] = jnp.zeros_like(total)

    def body(r0):
        at = pl.ds(r0, piece.step)
        also = pl.ds(rows + r0, piece.step)
        for k in range(piece.outer):
            re = piece.get(k, at, 0)
            if kind == "nonlinear":
                im = piece.get(k, at, 1)
                grads_out[k, at, :], grads_out[k, also, :] = re, im
                piece.put(k, at, 0, -0.5 * (re * re + im * im))
            elif kind == "residual":
                residual = re - target_p[k, also, :]
                total[...] += residual * residual
                piece.put(k, at, 0, residual)
            else:
                piece.put(k, at, 0, re * grads_in[k, at, :])
                piece.put(k, at, 1, re * grads_in[k, also, :])

    piece.chunks(body)
    piece.outgoing(-1.0, kind != "joint", out)
    if kind == "residual":
        value = 0.5 * jnp.sum(total[...])
        out[:, pl.ds(rows, 8), :] = jnp.full((out.shape[0], 8, 2 * rows), value, jnp.float32)


def member_step(device, field, target, forcing_p, constants, devices, rows, length):
    outer, inner = split_length(length)
    float32 = jnp.float32
    blocks = jax.ShapeDtypeStruct((devices, rows, 2 * rows), float32)
    longer = jax.ShapeDtypeStruct((devices, rows + 8, 2 * rows), float32)
    pair = jax.ShapeDtypeStruct((outer, 2 * rows, inner), float32)
    plain = jax.ShapeDtypeStruct((rows, length), float32)
    step = math.gcd(rows, 16)
    base = [
        pltpu.VMEM((2 * rows, length), float32),
        pltpu.VMEM((outer, rows, 2 * inner), jnp.bfloat16),
        pltpu.VMEM((outer, rows, 2 * inner), jnp.bfloat16),
        pltpu.VMEM((outer, rows, 2 * inner), float32),
    ]
    strided = pltpu.VMEM((length, TILE), float32)
    total = pltpu.VMEM((step, inner), float32)
    vmem = pl.BlockSpec(memory_space=pltpu.VMEM)
    smem = pl.BlockSpec(memory_space=pltpu.SMEM)

    def call(body, outs, scratch, *operands, scalar=False):
        specs = [smem if scalar and i == 0 else vmem for i in range(len(operands))]
        return pl.pallas_call(
            functools.partial(body, length, rows),
            out_shape=outs,
            in_specs=specs,
            out_specs=jax.tree.map(lambda leaf: vmem, outs),
            scratch_shapes=scratch,
            compiler_params=pltpu.CompilerParams(vmem_limit_bytes=48 * 2**20),
        )(*operands)

    def move(value):
        return lax.all_to_all(value, axes, split_axis=0, concat_axis=0, tiled=True)

    spectral = lambda kind: functools.partial(spectral_kernel, kind)
    physical = lambda kind: functools.partial(physical_kernel, kind)
    sent, target_p = call(start_kernel, (blocks, pair), base + [strided], field, target, *constants)
    sent, state = call(spectral("slope"), (blocks, pair), base, device, move(sent), *constants, scalar=True)
    sent, grads = call(physical("nonlinear"), (blocks, pair), base, move(sent), *constants)
    sent = call(spectral("next"), blocks, base, device, move(sent), state, forcing_p, *constants, scalar=True)
    sent, next_field = call(
        physical("residual"), (longer, plain), base + [strided, total], move(sent), target_p, *constants
    )
    sent, coef, sums = call(
        spectral("misfit"),
        (blocks, pair, jax.ShapeDtypeStruct((8, 2 * rows), float32)),
        base, device, move(sent), *constants, scalar=True,
    )
    sent = call(physical("joint"), blocks, base, move(sent), grads, *constants)
    sent = call(spectral("total"), blocks, base, device, move(sent), coef, *constants, scalar=True)
    field_grad = call(physical("last"), plain, base + [strided], move(sent), *constants)
    return next_field, sums[0, 0], field_grad, coef


def per_device(devices, initial_field, target_field, forcing):
    members, rows, length = initial_field.shape
    device = lax.axis_index(axes).astype(jnp.int32).reshape(1)
    constants = [jnp.asarray(table) for table in tables(length)]
    outer, inner = split_length(length)
    vmem = pl.BlockSpec(memory_space=pltpu.VMEM)
    strided = pltpu.VMEM((length, TILE), jnp.float32)

    def reorder(body, shape, operand):
        return pl.pallas_call(
            functools.partial(body, length, rows),
            out_shape=jax.ShapeDtypeStruct(shape, jnp.float32),
            in_specs=[vmem],
            out_specs=vmem,
            scratch_shapes=[strided],
        )(operand)

    forcing_p = reorder(spread_kernel, (outer, 2 * rows, inner), forcing)
    results = [
        member_step(device, initial_field[m], target_field[m], forcing_p, constants, devices, rows, length)
        for m in range(members)
    ]
    next_field = jnp.stack([one[0] for one in results])
    objective = sum(one[1] for one in results) / (members * length * length)
    field_grad = jnp.stack([one[2] for one in results])
    forcing_grad = reorder(collect_kernel, (2, rows, length), sum(one[3] for one in results))
    return (next_field, objective, field_grad, forcing_grad)


def solution(mesh):
    devices = mesh.shape["px"] * mesh.shape["py"]
    spec = P(None, axes, None)
    return jax.shard_map(
        functools.partial(per_device, devices),
        mesh=mesh,
        in_specs=(spec, spec, spec),
        out_specs=(spec, P(), spec, spec),
        check_vma=False,
    )
```

```python
import functools
import math

import jax
import jax.numpy as jnp
import numpy as np
from jax import lax
from jax.experimental import pallas as pl
from jax.experimental.pallas import tpu as pltpu
from jax.sharding import PartitionSpec as P

time_step = 0.25
axes = ("px", "py")
TILE = 128


def split_length(length):
    inner = 256 if length % 256 == 0 else TILE
    return (length // inner, inner)


def small_dft(items, sign):
    count = len(items)
    if count == 1:
        return items
    evens = small_dft(items[0::2], sign)
    odds = small_dft(items[1::2], sign)
    low, high = [], []
    for k in range(count // 2):
        odd_re, odd_im = odds[k]
        if 4 * k == count:
            odd_re, odd_im = (-odd_im, odd_re) if sign > 0 else (odd_im, -odd_re)
        elif k:
            c = math.cos(2.0 * math.pi * k / count)
            s = sign * math.sin(2.0 * math.pi * k / count)
            if abs(abs(c) - abs(s)) < 1e-12:
                sc, ss = math.copysign(1.0, c), math.copysign(1.0, s)
                odd_re, odd_im = (
                    c * (odd_re - sc * ss * odd_im),
                    c * (odd_im + sc * ss * odd_re),
                )
            else:
                odd_re, odd_im = (c * odd_re - s * odd_im, c * odd_im + s * odd_re)
        even_re, even_im = evens[k]
        low.append((even_re + odd_re, even_im + odd_im))
        high.append((even_re - odd_re, even_im - odd_im))
    return low + high


def halves(value):
    top = value.astype(jnp.bfloat16)
    return top, (value - top.astype(jnp.float32)).astype(jnp.bfloat16)


def orders(length, rows):
    inner = split_length(length)[1]
    half = rows // 2
    lane = np.arange(inner)
    natural = lane
    local = lane % (inner // 2)
    line = local % half
    kept = rows * (local // half) + np.where((lane >= inner // 2) & (line == 0), half, line)
    groups = TILE // rows
    tall = rows // groups
    within = lane % (inner // groups)
    lines = rows * (within // tall) + tall * (lane // (inner // groups)) + within % tall
    return natural, kept, lines


def twiddle_table(length, order):
    outer = split_length(length)[0]
    angle = 2.0 * np.pi * np.outer(np.arange(outer), order) / length
    return (np.stack([np.cos(angle), np.sin(angle)]) / math.sqrt(length)).astype(np.float32)


def matrix_table(length, sign, left, right):
    inner = split_length(length)[1]
    angle = 2.0 * np.pi * (np.outer(left, right) % inner) / inner
    c, s = np.cos(angle), np.sin(angle)
    full = np.block([[c, sign * s], [-sign * s, c]])
    top = full.astype(jnp.bfloat16)
    return np.stack([top, (full - top.astype(np.float64)).astype(jnp.bfloat16)])


def mirror_table(length):
    inner = split_length(length)[1]
    lane = np.arange(inner)
    both = np.zeros((2, inner, inner))
    both[0, (inner - lane) % inner, lane] = 1.0
    both[1, inner - 1 - lane, lane] = 1.0
    return both.astype(jnp.bfloat16)


class Pieces:
    def __init__(self, length, rows, turned=None, top=None, low=None, grid_out=None):
        self.length, self.rows, self.half = length, rows, rows // 2
        self.outer, self.inner = split_length(length)
        self.turned, self.top, self.low, self.z = turned, top, low, grid_out
        self.step = math.gcd(rows // 2, 16)

    def chunks(self, lines, body):
        def run(i, carry):
            body(pl.multiple_of(i * self.step, self.step))
            return carry

        lax.fori_loop(0, lines // self.step, run, 0)

    def put(self, k, at, part, value):
        lanes = pl.ds(part * self.inner, self.inner)
        top, low = halves(value)
        self.top[k, at, lanes] = top
        self.low[k, at, lanes] = low

    def get(self, k, at, part):
        return self.z[k, at, pl.ds(part * self.inner, self.inner)]

    def multiply(self, lines, matrix, real_in=False, real_out=False):
        deep = self.inner if real_in else 2 * self.inner
        wide = self.inner if real_out else 2 * self.inner
        count = self.outer * lines
        top = self.top[:, :lines, :deep].reshape(count, deep)
        low = self.low[:, :lines, :deep].reshape(count, deep)
        right_top = matrix[0, :deep, :wide]
        right_low = matrix[1, :deep, :wide]
        dot = functools.partial(jnp.dot, preferred_element_type=jnp.float32)
        total = dot(top, right_top) + dot(low, right_top) + dot(top, right_low)
        self.z[:, :lines, :wide] = total.reshape(self.outer, lines, wide)

    def twist(self, k, pair, sign, twiddle):
        c = twiddle[0, pl.ds(k, 1), :]
        s = twiddle[1, pl.ds(k, 1), :]
        s = s if sign > 0 else -s
        re, im = pair
        return (re * c - im * s, re * s + im * c)

    def turn_full(self, source):
        rows, blocks = self.rows, TILE // self.rows
        for t in range(self.length // TILE):
            tile = source[pl.ds(t * blocks, blocks), :rows, :].reshape(TILE, 2 * rows)
            self.turned[: 2 * rows, pl.ds(t * TILE, TILE)] = tile.T

    def turn_lines(self, source):
        rows = self.rows
        groups = TILE // rows
        blocks, wide = self.inner // rows, self.inner // groups
        for t in range(self.outer):
            tile = source[pl.ds(t * blocks, blocks), :, :].reshape(wide, TILE).T
            for h in range(groups):
                self.turned[:rows, pl.ds(t * self.inner + h * wide, wide)] = tile[h * rows : (h + 1) * rows]

    def kept_lanes(self, j):
        wide = self.inner // 2
        return j * self.inner + (wide if 2 * j >= self.outer else 0), wide

    def clear_other(self, j):
        at, wide = self.kept_lanes(j)
        other = j * self.inner + (0 if 2 * j >= self.outer else wide)
        self.turned[: 2 * self.rows, pl.ds(other, wide)] = jnp.zeros((2 * self.rows, wide), jnp.float32)

    def turn_kept(self, source):
        rows, half, blocks = self.rows, self.half, self.inner // self.rows
        for j in range(self.outer):
            at, wide = self.kept_lanes(j)
            tile = source[pl.ds(j * blocks, blocks), :, :].reshape(wide, 2 * rows)
            self.turned[: 2 * rows, pl.ds(at, wide)] = tile.T
            self.clear_other(j)

    def unpack_middle(self):
        rows, middle = self.rows, (self.outer // 2) * self.inner
        first = self.turned[rows : 2 * rows, :TILE]
        lane0 = lax.broadcasted_iota(jnp.int32, first.shape, 1) == 0
        zero = jnp.zeros_like(first)
        self.turned[:rows, pl.ds(middle, TILE)] += jnp.where(lane0, first, zero)
        self.turned[rows : 2 * rows, :TILE] = jnp.where(lane0, zero, first)

    def incoming(self, lines, sign, twiddle, matrix, real_out=False):
        def body(r0):
            items = []
            for j in range(self.outer):
                lanes = pl.ds(j * self.inner, self.inner)
                items.append((
                    self.turned[pl.ds(r0, self.step), lanes],
                    self.turned[pl.ds(lines + r0, self.step), lanes],
                ))
            for k, pair in enumerate(small_dft(items, sign)):
                re, im = self.twist(k, pair, sign, twiddle)
                self.put(k, pl.ds(r0, self.step), 0, re)
                self.put(k, pl.ds(r0, self.step), 1, im)

        self.chunks(lines, body)
        self.multiply(lines, matrix, real_out=real_out)

    def outgoing(self, lines, sign, twiddle, matrix, real_in, write):
        self.multiply(lines, matrix, real_in=real_in)

        def body(r0):
            at = pl.ds(r0, self.step)
            write(r0, small_dft([
                self.twist(k, (self.get(k, at, 0), self.get(k, at, 1)), sign, twiddle)
                for k in range(self.outer)
            ], sign))

        self.chunks(lines, body)

    def pack_middle(self, items):
        re, im = items[0]
        lane0 = lax.broadcasted_iota(jnp.int32, im.shape, 1) == 0
        return [(re, jnp.where(lane0, items[self.outer // 2][0], im))] + items[1:]

    def write_full(self, result, pack):
        rows = self.rows

        def write(r0, items):
            at = pl.ds(r0, self.step)
            for j, (re, im) in enumerate(self.pack_middle(items) if pack else items):
                for piece in range(self.inner // rows):
                    to = j * (self.inner // rows) + piece
                    lanes = slice(piece * rows, (piece + 1) * rows)
                    result[to, at, pl.ds(0, rows)] = re[:, lanes]
                    result[to, at, pl.ds(rows, rows)] = im[:, lanes]

        return write

    def outgoing_kept(self, twiddle, matrix, result):
        self.multiply(self.rows, matrix, real_in=True)
        rows, half, blocks = self.rows, self.half, self.inner // self.rows
        tall = rows * rows // TILE
        step = math.gcd(rows, 16)
        span = min(tall, step)
        for h in range(rows // max(tall, step)):

            def body(i, carry, h=h):
                r0 = i * step if isinstance(i, int) else pl.multiple_of(i * step, step)
                at = pl.ds(h * max(tall, step) + r0, step)
                items = self.pack_middle(small_dft([
                    self.twist(k, (self.get(k, at, 0), self.get(k, at, 1)), -1.0, twiddle)
                    for k in range(self.outer)
                ], -1.0))
                for j, pair in enumerate(items):
                    base = self.inner // 2 if 2 * j >= self.outer else 0
                    for piece in range(blocks):
                        lanes = slice(base + piece * half, base + (piece + 1) * half)
                        for part, value in enumerate(pair):
                            for sub in range(step // span):
                                group = h * (step // span) + sub
                                to = pl.ds(group * rows + part * half, half)
                                held = value[sub * span : (sub + 1) * span, lanes]
                                result[j * blocks + piece, pl.ds(r0, span), to] = held
                return carry

            if tall > step:
                lax.fori_loop(0, tall // step, body, 0)
            else:
                body(0, 0)

    def mirrored(self, blocks, mirror):
        dot = functools.partial(jnp.dot, preferred_element_type=jnp.float32)

        def flip(values, which):
            top, low = halves(jnp.concatenate(values, axis=0))
            return dot(top, mirror[which]) + dot(low, mirror[which])

        flat = [part for k in range(self.outer) for pair in blocks[k] for part in pair]
        per = 2 * len(blocks[0])
        low = flip(flat[:per], 0)
        high = flip(flat[per:], 1)
        out = []
        for k in range(self.outer):
            part, base = (low, 0) if k == 0 else (high, (self.outer - k - 1) * per)
            take = lambda i: part[(base + i) * 8 : (base + i + 1) * 8]
            out.append([(take(2 * i), -take(2 * i + 1)) for i in range(per // 2)])
        return out

    def spread(self, first, second, strided, result):
        rows, fill = self.rows, TILE - 2 * self.rows
        for t in range(self.length // TILE):
            lanes = pl.ds(t * TILE, TILE)
            parts = [first[:, lanes], second[:, lanes]]
            if fill:
                parts.append(jnp.zeros((fill, TILE), jnp.float32))
            strided[pl.ds(t * TILE, TILE), :] = jnp.concatenate(parts, axis=0).T
        for k in range(self.outer):
            slab = strided[pl.ds(k, self.inner, stride=self.outer), :].T
            result[k] = slab[: 2 * rows, :]

    def collect(self, slabs, strided, results):
        rows = self.rows
        for k in range(self.outer):
            slab = slabs(k)
            fill = TILE - slab.shape[0]
            if fill:
                slab = jnp.concatenate([slab, jnp.zeros((fill, self.inner), jnp.float32)], axis=0)
            strided[pl.ds(k, self.inner, stride=self.outer), :] = slab.T
        for t in range(self.length // TILE):
            block = strided[pl.ds(t * TILE, TILE), :].T
            for i, result in enumerate(results):
                result[:, pl.ds(t * TILE, TILE)] = block[i * rows : (i + 1) * rows, :]


def signed_waves(position, count):
    signed = jnp.where(position < count // 2, position, position - count)
    waves = 4.0 * signed.astype(jnp.float32) / count
    return waves, jnp.where(position == count // 2, jnp.float32(0.0), waves)


def first_waves(piece, k):
    lanes = lax.broadcasted_iota(jnp.int32, (1, piece.inner), 1)
    return signed_waves(piece.outer * lanes + k, piece.length)


def inverse_denominator(wave_first, wave_second):
    square = wave_first * wave_first + wave_second * wave_second
    return 1.0 / (1.0 + time_step * (square * square - square))


def second_wave(piece, position):
    shape = (position.shape[0], piece.inner)
    return jnp.broadcast_to(signed_waves(position, piece.length)[0], shape)


def row_index(count, width):
    return lax.broadcasted_iota(jnp.int32, (count, width), 0)


def start_kernel(length, rows, field, target, twiddle, matrix, out, both_p, *scratch):
    piece = Pieces(length, rows, *scratch[:4])
    piece.spread(field, target, scratch[4], both_p)

    def body(r0):
        at = pl.ds(r0, piece.step)
        for k in range(piece.outer):
            piece.put(k, at, 0, both_p[k, at, :])

    piece.chunks(rows, body)
    piece.outgoing_kept(twiddle, matrix, out)


def slope_second_kernel(length, rows, field_p, twiddle, out_matrix, in_matrix, kept, result, *scratch):
    piece = Pieces(length, rows, *scratch)

    def body(r0):
        at = pl.ds(r0, piece.step)
        for k in range(piece.outer):
            piece.put(k, at, 0, field_p[k, at, :])

    piece.chunks(rows, body)
    for j in range(piece.outer):
        piece.clear_other(j)

    def write(r0, items):
        for j, (re, im) in enumerate(items):
            at, wide = piece.kept_lanes(j)
            base = at - j * piece.inner
            position = j * piece.inner + kept[:, base : base + wide]
            slope = 2.0 * signed_waves(position, length)[1]
            piece.turned[pl.ds(r0, piece.step), pl.ds(at, wide)] = -slope * im[:, base : base + wide]
            piece.turned[pl.ds(rows + r0, piece.step), pl.ds(at, wide)] = slope * re[:, base : base + wide]

    piece.outgoing(rows, -1.0, twiddle, out_matrix, True, write)
    piece.incoming(rows, 1.0, twiddle, in_matrix, real_out=True)
    result[...] = piece.z[:, :, : piece.inner]


def spread_kernel(length, rows, forcing, result, strided):
    Pieces(length, rows).spread(forcing.at[0], forcing.at[1], strided, result)


def collect_kernel(length, rows, slabs, result, strided):
    piece = Pieces(length, rows)
    piece.collect(lambda k: slabs[k], strided, [result.at[i] for i in range(result.shape[0])])


def weight_of(device, r0, step, inner):
    alone = (row_index(step, inner) + r0 + device) == 0
    return jnp.where(alone, jnp.float32(1.0), jnp.float32(2.0))


def slope_kernel(length, rows, device_ref, source, in_twiddle, in_matrix, out_twiddle, out_matrix, out, state, *scratch):
    device = device_ref[0]
    piece = Pieces(length, rows, *scratch)
    half = piece.half
    piece.turn_lines(source)
    piece.incoming(half, -1.0, in_twiddle, in_matrix)

    def body(r0):
        at, also = pl.ds(r0, piece.step), pl.ds(half + r0, piece.step)
        weight = weight_of(device, r0, piece.step, piece.inner)
        for k in range(piece.outer):
            re, im = piece.get(k, at, 0), piece.get(k, at, 1)
            state[k, at, :], state[k, also, :] = re, im
            scale = first_waves(piece, k)[1] * weight
            piece.put(k, at, 0, -scale * im)
            piece.put(k, at, 1, scale * re)

    piece.chunks(half, body)
    piece.outgoing(half, 1.0, out_twiddle, out_matrix, False, piece.write_full(out, False))


def total_kernel(length, rows, device_ref, source, coef, in_twiddle, in_matrix, out_twiddle, out_matrix, out, *scratch):
    device = device_ref[0]
    piece = Pieces(length, rows, *scratch)
    half = piece.half
    piece.turn_lines(source)
    piece.incoming(half, -1.0, in_twiddle, in_matrix)

    def body(r0):
        at, also = pl.ds(r0, piece.step), pl.ds(half + r0, piece.step)
        weight = weight_of(device, r0, piece.step, piece.inner)
        for k in range(piece.outer):
            re, im = piece.get(k, at, 0), piece.get(k, at, 1)
            deriv = first_waves(piece, k)[1]
            scale = 1.0 / time_step
            piece.put(k, at, 0, weight * (scale * coef[k, at, :] - deriv * im))
            piece.put(k, at, 1, weight * (scale * coef[k, also, :] + deriv * re))

    piece.chunks(half, body)
    piece.outgoing(half, 1.0, out_twiddle, out_matrix, False, piece.write_full(out, False))


def edge_inverses(piece, k):
    wave_first = first_waves(piece, k)[0]
    middle = jnp.full((1, 1), piece.length // 2, jnp.int32)
    zero = jnp.zeros((1, 1), jnp.int32)
    return [inverse_denominator(wave_first, signed_waves(p, piece.length)[0]) for p in (zero, middle)]


def next_kernel(length, rows, device_ref, source, state, forcing, in_twiddle, in_matrix, out_twiddle, out_matrix, mirror, out, *scratch):
    device = device_ref[0]
    piece = Pieces(length, rows, *scratch)
    half, step, inner = piece.half, piece.step, piece.inner
    late = device >= (length // rows) // 2
    piece.turn_lines(source)
    piece.incoming(half, -1.0, in_twiddle, in_matrix)

    def body(r0):
        at, also = pl.ds(r0, step), pl.ds(half + r0, step)
        index = row_index(step, 1) + r0
        low_wave = second_wave(piece, device * rows + index)
        high_wave = second_wave(piece, device * rows + half + index)
        moved = jnp.logical_and(row_index(step, inner) + r0 == 0, late)
        weight = weight_of(device, r0, step, inner)
        for k in range(piece.outer):
            wave_first = first_waves(piece, k)[0]
            low = inverse_denominator(wave_first, low_wave)
            high = inverse_denominator(wave_first, high_wave)
            for part in range(2):
                own = state[k, pl.ds(part * half + r0, step), :] + time_step * piece.get(k, at, part)
                own = weight * own
                f_low = time_step * forcing[k, pl.ds(part * rows + r0, step), :]
                f_high = time_step * forcing[k, pl.ds(part * rows + half + r0, step), :]
                piece.put(k, at, part, (f_low + jnp.where(moved, 0.0, own)) * low)
                piece.put(k, also, part, (f_high + jnp.where(moved, own, 0.0)) * high)

    piece.chunks(half, body)

    @pl.when(device == 0)
    def _():
        at = pl.ds(0, 8)
        blocks = []
        for k in range(piece.outer):
            own = tuple(
                state[k, pl.ds(part * half, 8), :] + time_step * piece.get(k, at, part) for part in range(2)
            )
            full = tuple(
                own[part] + time_step * forcing[k, pl.ds(part * rows, 8), :] for part in range(2)
            )
            blocks.append([own, full])
        flipped = piece.mirrored(blocks, mirror)
        rest = pl.ds(0, 16)
        row0 = row_index(16, inner) == 0
        for k in range(piece.outer):
            zero, middle = edge_inverses(piece, k)
            for part in range(2):
                own, full = blocks[k][0][part], blocks[k][1][part]
                own_c, full_c = flipped[k][0][part], flipped[k][1][part]
                value = 0.5 * ((full + full_c) * zero + (own - own_c) * middle)
                replace(piece, k, part, value)

    piece.outgoing(rows, 1.0, out_twiddle, out_matrix, False, piece.write_full(out, False))


def replace(piece, k, part, value):
    lanes = pl.ds(part * piece.inner, piece.inner)
    row0 = row_index(16, piece.inner) == 0
    value = jnp.concatenate([value, value], axis=0)
    for held, new in zip((piece.top, piece.low), halves(value)):
        old = held[k, pl.ds(0, 16), lanes].astype(jnp.float32)
        held[k, pl.ds(0, 16), lanes] = jnp.where(row0, new.astype(jnp.float32), old).astype(jnp.bfloat16)


def misfit_kernel(length, rows, device_ref, source, in_twiddle, in_matrix, out_twiddle, out_matrix, mirror, out, full, coef, total_out, *scratch):
    device = device_ref[0]
    piece = Pieces(length, rows, *scratch)
    half, step, inner = piece.half, piece.step, piece.inner
    late = device >= (length // rows) // 2
    piece.turn_full(source)
    piece.incoming(rows, -1.0, in_twiddle, in_matrix)

    def body(r0):
        at, also = pl.ds(r0, step), pl.ds(half + r0, step)
        index = row_index(step, 1) + r0
        low_wave = second_wave(piece, device * rows + index)
        high_wave = second_wave(piece, device * rows + half + index)
        moved = jnp.logical_and(row_index(step, inner) + r0 == 0, late)
        weight = weight_of(device, r0, step, inner)
        for k in range(piece.outer):
            wave_first = first_waves(piece, k)[0]
            low = time_step * inverse_denominator(wave_first, low_wave)
            high = time_step * inverse_denominator(wave_first, high_wave)
            for part in range(2):
                low_value = piece.get(k, at, part) * low
                high_value = piece.get(k, also, part) * high
                full[k, pl.ds(part * rows + r0, step), :] = low_value
                full[k, pl.ds(part * rows + half + r0, step), :] = high_value
                own = jnp.where(moved, high_value, low_value)
                coef[k, pl.ds(part * half + r0, step), :] = own
                piece.put(k, at, part, weight * own)

    piece.chunks(half, body)

    @pl.when(device == 0)
    def _():
        at = pl.ds(0, 8)
        blocks = [[(piece.get(k, at, 0), piece.get(k, at, 1))] for k in range(piece.outer)]
        flipped = piece.mirrored(blocks, mirror)
        row0 = row_index(8, inner) == 0
        for k in range(piece.outer):
            zero, middle = edge_inverses(piece, k)
            for part in range(2):
                own, own_c = blocks[k][0][part], flipped[k][0][part]
                first = (0.5 * time_step) * (own + own_c) * zero
                value = first + (0.5 * time_step) * (own - own_c) * middle
                at_full, at_coef = pl.ds(part * rows, 8), pl.ds(part * half, 8)
                full[k, at_full, :] = jnp.where(row0, first, full[k, at_full, :])
                coef[k, at_coef, :] = jnp.where(row0, value, coef[k, at_coef, :])
                replace(piece, k, part, value)

    piece.outgoing(half, 1.0, out_twiddle, out_matrix, False, piece.write_full(out, False))
    total_out[...] = jnp.sum(source[:, pl.ds(rows, 8), :], axis=0)


def nonlinear_kernel(length, rows, source, second, twiddle, in_matrix, out_matrix, out, first_out, *scratch):
    piece = Pieces(length, rows, *scratch)
    piece.turn_kept(source)
    piece.unpack_middle()
    piece.incoming(rows, 1.0, twiddle, in_matrix, real_out=True)

    def body(r0):
        at = pl.ds(r0, piece.step)
        for k in range(piece.outer):
            first, other = piece.get(k, at, 0), second[k, at, :]
            first_out[k, at, :] = first
            piece.put(k, at, 0, -0.5 * (first * first + other * other))

    piece.chunks(rows, body)
    piece.outgoing_kept(twiddle, out_matrix, out)


def joint_kernel(length, rows, source, first, second, twiddle, in_matrix, out_matrix, out, second_out, *scratch):
    piece = Pieces(length, rows, *scratch)
    piece.turn_kept(source)
    piece.unpack_middle()
    piece.incoming(rows, 1.0, twiddle, in_matrix, real_out=True)

    def body(r0):
        at = pl.ds(r0, piece.step)
        for k in range(piece.outer):
            value = piece.get(k, at, 0)
            second_out[k, at, :] = value * second[k, at, :]
            piece.put(k, at, 0, value * first[k, at, :])

    piece.chunks(rows, body)
    piece.outgoing_kept(twiddle, out_matrix, out)


def residual_kernel(length, rows, source, both_p, twiddle, in_matrix, out_matrix, out, field_out, *scratch):
    piece = Pieces(length, rows, *scratch[:4])
    strided, total = scratch[4:]
    piece.turn_full(source)
    piece.unpack_middle()
    piece.incoming(rows, 1.0, twiddle, in_matrix, real_out=True)
    piece.collect(lambda k: piece.get(k, pl.ds(0, rows), 0), strided, [field_out])
    total[...] = jnp.zeros_like(total)

    def body(r0):
        at = pl.ds(r0, piece.step)
        for k in range(piece.outer):
            residual = piece.get(k, at, 0) - both_p[k, pl.ds(rows + r0, piece.step), :]
            total[...] += residual * residual
            piece.put(k, at, 0, residual)

    piece.chunks(rows, body)
    piece.outgoing(rows, -1.0, twiddle, out_matrix, True, piece.write_full(out, True))
    value = 0.5 * jnp.sum(total[...])
    out[:, pl.ds(rows, 8), :] = jnp.full((out.shape[0], 8, 2 * rows), value, jnp.float32)


def last_kernel(length, rows, source, second, twiddle, in_matrix, field_out, *scratch):
    piece = Pieces(length, rows, *scratch[:4])
    piece.turn_kept(source)
    piece.unpack_middle()
    piece.incoming(rows, 1.0, twiddle, in_matrix, real_out=True)
    piece.collect(
        lambda k: piece.get(k, pl.ds(0, rows), 0) + second[k], scratch[4], [field_out]
    )


def member_step(device, field, target, forcing_p, devices, rows, length):
    outer, inner = split_length(length)
    half = rows // 2
    float32 = jnp.float32
    shape = lambda *dims: jax.ShapeDtypeStruct(dims, float32)
    kept_blocks = shape(devices, rows * rows // TILE, TILE)
    half_blocks = shape(devices, half, 2 * rows)
    blocks = shape(devices, rows, 2 * rows)
    longer = shape(devices, rows + 8, 2 * rows)
    pair, one = shape(outer, 2 * rows, inner), shape(outer, rows, inner)
    plain = shape(rows, length)
    step = math.gcd(half, 16)
    base = [
        pltpu.VMEM((2 * rows, length), float32),
        pltpu.VMEM((outer, rows, 2 * inner), jnp.bfloat16),
        pltpu.VMEM((outer, rows, 2 * inner), jnp.bfloat16),
        pltpu.VMEM((outer, rows, 2 * inner), float32),
    ]
    strided = pltpu.VMEM((length, TILE), float32)
    total = pltpu.VMEM((step, inner), float32)
    vmem = pl.BlockSpec(memory_space=pltpu.VMEM)
    smem = pl.BlockSpec(memory_space=pltpu.SMEM)

    natural, kept, lines = orders(length, rows)
    tw_natural, tw_kept, tw_lines = [jnp.asarray(twiddle_table(length, o)) for o in (natural, kept, lines)]
    matrix = lambda *args: jnp.asarray(matrix_table(length, *args))
    forward, backward = matrix(-1.0, natural, natural), matrix(1.0, natural, natural)
    kept_out, kept_in = matrix(-1.0, natural, kept), matrix(1.0, kept, natural)
    lines_in = matrix(-1.0, lines, natural)
    mirror = jnp.asarray(mirror_table(length))
    kept_lane = jnp.asarray(kept[None, :].astype(np.int32))

    def call(body, outs, scratch, *operands):
        return pl.pallas_call(
            functools.partial(body, length, rows),
            out_shape=outs,
            in_specs=[smem if operand is device else vmem for operand in operands],
            out_specs=jax.tree.map(lambda leaf: vmem, outs),
            scratch_shapes=scratch,
            compiler_params=pltpu.CompilerParams(vmem_limit_bytes=48 * 2**20),
            cost_estimate=pl.CostEstimate(flops=6 * 10**9, bytes_accessed=4 * 2**20, transcendentals=0),
        )(*operands)

    def move(value):
        return lax.all_to_all(value, axes, split_axis=0, concat_axis=0, tiled=True)

    spectral_tables = (tw_lines, lines_in, tw_natural, backward)
    slope_tables = (tw_kept, kept_out, kept_in, kept_lane)
    sent, both_p = call(start_kernel, (kept_blocks, pair), base + [strided], field, target, tw_kept, kept_out)
    second = call(slope_second_kernel, one, base, both_p, *slope_tables)
    sent, state = call(slope_kernel, (half_blocks, one), base, device, move(sent), *spectral_tables)
    sent, first = call(nonlinear_kernel, (kept_blocks, one), base, move(sent), second, tw_kept, kept_in, kept_out)
    sent = call(next_kernel, blocks, base, device, move(sent), state, forcing_p, *spectral_tables, mirror)
    sent, next_field = call(
        residual_kernel, (longer, plain), base + [strided, total],
        move(sent), both_p, tw_natural, backward, forward,
    )
    sent, full, coef, sums = call(
        misfit_kernel, (half_blocks, pair, one, shape(8, 2 * rows)), base,
        device, move(sent), tw_natural, forward, tw_natural, backward, mirror,
    )
    sent, product = call(
        joint_kernel, (kept_blocks, one), base, move(sent), first, second, tw_kept, kept_in, kept_out
    )
    second_part = call(slope_second_kernel, one, base, product, *slope_tables)
    sent = call(total_kernel, half_blocks, base, device, move(sent), coef, *spectral_tables)
    field_grad = call(last_kernel, plain, base + [strided], move(sent), second_part, tw_kept, kept_in)
    return next_field, sums[0, 0], field_grad, full


def per_device(devices, initial_field, target_field, forcing):
    members, rows, length = initial_field.shape
    device = lax.axis_index(axes).astype(jnp.int32).reshape(1)
    outer, inner = split_length(length)
    vmem = pl.BlockSpec(memory_space=pltpu.VMEM)
    strided = pltpu.VMEM((length, TILE), jnp.float32)

    def reorder(body, shape, operand):
        return pl.pallas_call(
            functools.partial(body, length, rows),
            out_shape=jax.ShapeDtypeStruct(shape, jnp.float32),
            in_specs=[vmem],
            out_specs=vmem,
            scratch_shapes=[strided],
        )(operand)

    forcing_p = reorder(spread_kernel, (outer, 2 * rows, inner), forcing)
    results = [
        member_step(device, initial_field[m], target_field[m], forcing_p, devices, rows, length)
        for m in range(members)
    ]
    next_field = jnp.stack([one[0] for one in results])
    objective = sum(one[1] for one in results) / (members * length * length)
    field_grad = jnp.stack([one[2] for one in results])
    forcing_grad = reorder(collect_kernel, (2, rows, length), sum(one[3] for one in results))
    return (next_field, objective, field_grad, forcing_grad)


def solution(mesh):
    devices = mesh.shape["px"] * mesh.shape["py"]
    spec = P(None, axes, None)
    return jax.shard_map(
        functools.partial(per_device, devices),
        mesh=mesh,
        in_specs=(spec, spec, spec),
        out_specs=(spec, P(), spec, spec),
        check_vma=False,
    )
```

```python
import functools
import math

import jax
import jax.numpy as jnp
import numpy as np
from jax import lax
from jax.experimental import pallas as pl
from jax.experimental.pallas import tpu as pltpu
from jax.sharding import PartitionSpec as P

time_step = 0.25
axes = ("px", "py")
TILE = 128


def split_length(length):
    inner = 256 if length % 256 == 0 else TILE
    return (length // inner, inner)


def small_dft(items, sign):
    count = len(items)
    if count == 1:
        return items
    evens = small_dft(items[0::2], sign)
    odds = small_dft(items[1::2], sign)
    low, high = [], []
    for k in range(count // 2):
        odd_re, odd_im = odds[k]
        if 4 * k == count:
            odd_re, odd_im = (-odd_im, odd_re) if sign > 0 else (odd_im, -odd_re)
        elif k:
            c = math.cos(2.0 * math.pi * k / count)
            s = sign * math.sin(2.0 * math.pi * k / count)
            if abs(abs(c) - abs(s)) < 1e-12:
                sc, ss = math.copysign(1.0, c), math.copysign(1.0, s)
                odd_re, odd_im = (
                    c * (odd_re - sc * ss * odd_im),
                    c * (odd_im + sc * ss * odd_re),
                )
            else:
                odd_re, odd_im = (c * odd_re - s * odd_im, c * odd_im + s * odd_re)
        even_re, even_im = evens[k]
        low.append((even_re + odd_re, even_im + odd_im))
        high.append((even_re - odd_re, even_im - odd_im))
    return low + high


def halves(value):
    top = value.astype(jnp.bfloat16)
    return top, (value - top.astype(jnp.float32)).astype(jnp.bfloat16)


def orders(length, rows):
    inner = split_length(length)[1]
    half = rows // 2
    lane = np.arange(inner)
    natural = lane
    local = lane % (inner // 2)
    line = local % half
    kept = rows * (local // half) + np.where((lane >= inner // 2) & (line == 0), half, line)
    groups = TILE // rows
    tall = rows // groups
    within = lane % (inner // groups)
    lines = rows * (within // tall) + tall * (lane // (inner // groups)) + within % tall
    return natural, kept, lines


def twiddle_table(length, order):
    outer = split_length(length)[0]
    angle = 2.0 * np.pi * np.outer(np.arange(outer), order) / length
    return (np.stack([np.cos(angle), np.sin(angle)]) / math.sqrt(length)).astype(np.float32)


def matrix_table(length, sign, left, right):
    inner = split_length(length)[1]
    angle = 2.0 * np.pi * (np.outer(left, right) % inner) / inner
    c, s = np.cos(angle), np.sin(angle)
    full = np.block([[c, sign * s], [-sign * s, c]])
    top = full.astype(jnp.bfloat16)
    return np.stack([top, (full - top.astype(np.float64)).astype(jnp.bfloat16)])


def mirror_table(length):
    inner = split_length(length)[1]
    lane = np.arange(inner)
    both = np.zeros((2, inner, inner))
    both[0, (inner - lane) % inner, lane] = 1.0
    both[1, inner - 1 - lane, lane] = 1.0
    return both.astype(jnp.bfloat16)


class Pieces:
    def __init__(self, length, rows, turned=None, top=None, low=None, grid_out=None):
        self.length, self.rows, self.half = length, rows, rows // 2
        self.outer, self.inner = split_length(length)
        self.turned, self.top, self.low, self.z = turned, top, low, grid_out
        self.step = math.gcd(rows // 2, 16)

    def chunks(self, lines, body):
        def run(i, carry):
            body(pl.multiple_of(i * self.step, self.step))
            return carry

        lax.fori_loop(0, lines // self.step, run, 0)

    def put(self, k, at, part, value):
        lanes = pl.ds(part * self.inner, self.inner)
        top, low = halves(value)
        self.top[k, at, lanes] = top
        self.low[k, at, lanes] = low

    def get(self, k, at, part):
        return self.z[k, at, pl.ds(part * self.inner, self.inner)]

    def multiply(self, lines, matrix, real_in=False, real_out=False):
        deep = self.inner if real_in else 2 * self.inner
        wide = self.inner if real_out else 2 * self.inner
        count = self.outer * lines
        top = self.top[:, :lines, :deep].reshape(count, deep)
        low = self.low[:, :lines, :deep].reshape(count, deep)
        right_top = matrix[0, :deep, :wide]
        right_low = matrix[1, :deep, :wide]
        dot = functools.partial(jnp.dot, preferred_element_type=jnp.float32)
        total = dot(top, right_top) + dot(low, right_top) + dot(top, right_low)
        self.z[:, :lines, :wide] = total.reshape(self.outer, lines, wide)

    def twist(self, k, pair, sign, twiddle):
        c = twiddle[0, pl.ds(k, 1), :]
        s = twiddle[1, pl.ds(k, 1), :]
        s = s if sign > 0 else -s
        re, im = pair
        return (re * c - im * s, re * s + im * c)

    def turn_full(self, source):
        rows, blocks = self.rows, TILE // self.rows
        for t in range(self.length // TILE):
            tile = source[pl.ds(t * blocks, blocks), :rows, :].reshape(TILE, 2 * rows)
            self.turned[: 2 * rows, pl.ds(t * TILE, TILE)] = tile.T

    def turn_lines(self, source):
        rows = self.rows
        groups = TILE // rows
        blocks, wide = self.inner // rows, self.inner // groups
        for t in range(self.outer):
            tile = source[pl.ds(t * blocks, blocks), :, :].reshape(wide, TILE).T
            for h in range(groups):
                self.turned[:rows, pl.ds(t * self.inner + h * wide, wide)] = tile[h * rows : (h + 1) * rows]

    def kept_lanes(self, j):
        wide = self.inner // 2
        return j * self.inner + (wide if 2 * j >= self.outer else 0), wide

    def clear_other(self, j):
        at, wide = self.kept_lanes(j)
        other = j * self.inner + (0 if 2 * j >= self.outer else wide)
        self.turned[: 2 * self.rows, pl.ds(other, wide)] = jnp.zeros((2 * self.rows, wide), jnp.float32)

    def turn_kept(self, source):
        rows, half, blocks = self.rows, self.half, self.inner // self.rows
        for j in range(self.outer):
            at, wide = self.kept_lanes(j)
            tile = source[pl.ds(j * blocks, blocks), :, :].reshape(wide, 2 * rows)
            self.turned[: 2 * rows, pl.ds(at, wide)] = tile.T
            self.clear_other(j)

    def unpack_middle(self):
        rows, middle = self.rows, (self.outer // 2) * self.inner
        first = self.turned[rows : 2 * rows, :TILE]
        lane0 = lax.broadcasted_iota(jnp.int32, first.shape, 1) == 0
        zero = jnp.zeros_like(first)
        self.turned[:rows, pl.ds(middle, TILE)] += jnp.where(lane0, first, zero)
        self.turned[rows : 2 * rows, :TILE] = jnp.where(lane0, zero, first)

    def incoming(self, lines, sign, twiddle, matrix, real_out=False):
        def body(r0):
            items = []
            for j in range(self.outer):
                lanes = pl.ds(j * self.inner, self.inner)
                items.append((
                    self.turned[pl.ds(r0, self.step), lanes],
                    self.turned[pl.ds(lines + r0, self.step), lanes],
                ))
            for k, pair in enumerate(small_dft(items, sign)):
                re, im = self.twist(k, pair, sign, twiddle)
                self.put(k, pl.ds(r0, self.step), 0, re)
                self.put(k, pl.ds(r0, self.step), 1, im)

        self.chunks(lines, body)
        self.multiply(lines, matrix, real_out=real_out)

    def outgoing(self, lines, sign, twiddle, matrix, real_in, write):
        self.multiply(lines, matrix, real_in=real_in)

        def body(r0):
            at = pl.ds(r0, self.step)
            write(r0, small_dft([
                self.twist(k, (self.get(k, at, 0), self.get(k, at, 1)), sign, twiddle)
                for k in range(self.outer)
            ], sign))

        self.chunks(lines, body)

    def pack_middle(self, items):
        re, im = items[0]
        lane0 = lax.broadcasted_iota(jnp.int32, im.shape, 1) == 0
        return [(re, jnp.where(lane0, items[self.outer // 2][0], im))] + items[1:]

    def write_full(self, result, pack):
        rows = self.rows

        def write(r0, items):
            at = pl.ds(r0, self.step)
            for j, (re, im) in enumerate(self.pack_middle(items) if pack else items):
                for piece in range(self.inner // rows):
                    to = j * (self.inner // rows) + piece
                    lanes = slice(piece * rows, (piece + 1) * rows)
                    result[to, at, pl.ds(0, rows)] = re[:, lanes]
                    result[to, at, pl.ds(rows, rows)] = im[:, lanes]

        return write

    def outgoing_kept(self, twiddle, matrix, result):
        self.multiply(self.rows, matrix, real_in=True)
        rows, half, blocks = self.rows, self.half, self.inner // self.rows
        tall = rows * rows // TILE
        step = math.gcd(rows, 16)
        span = min(tall, step)
        for h in range(rows // max(tall, step)):

            def body(i, carry, h=h):
                r0 = i * step if isinstance(i, int) else pl.multiple_of(i * step, step)
                at = pl.ds(h * max(tall, step) + r0, step)
                items = self.pack_middle(small_dft([
                    self.twist(k, (self.get(k, at, 0), self.get(k, at, 1)), -1.0, twiddle)
                    for k in range(self.outer)
                ], -1.0))
                for j, pair in enumerate(items):
                    base = self.inner // 2 if 2 * j >= self.outer else 0
                    for piece in range(blocks):
                        lanes = slice(base + piece * half, base + (piece + 1) * half)
                        for part, value in enumerate(pair):
                            for sub in range(step // span):
                                group = h * (step // span) + sub
                                to = pl.ds(group * rows + part * half, half)
                                held = value[sub * span : (sub + 1) * span, lanes]
                                result[j * blocks + piece, pl.ds(r0, span), to] = held
                return carry

            if tall > step:
                lax.fori_loop(0, tall // step, body, 0)
            else:
                body(0, 0)

    def mirrored(self, blocks, mirror):
        dot = functools.partial(jnp.dot, preferred_element_type=jnp.float32)

        def flip(values, which):
            top, low = halves(jnp.concatenate(values, axis=0))
            return dot(top, mirror[which]) + dot(low, mirror[which])

        flat = [part for k in range(self.outer) for pair in blocks[k] for part in pair]
        per = 2 * len(blocks[0])
        low = flip(flat[:per], 0)
        high = flip(flat[per:], 1)
        out = []
        for k in range(self.outer):
            part, base = (low, 0) if k == 0 else (high, (self.outer - k - 1) * per)
            take = lambda i: part[(base + i) * 8 : (base + i + 1) * 8]
            out.append([(take(2 * i), -take(2 * i + 1)) for i in range(per // 2)])
        return out

    def spread(self, first, second, strided, result):
        rows, fill = self.rows, TILE - 2 * self.rows
        for t in range(self.length // TILE):
            lanes = pl.ds(t * TILE, TILE)
            parts = [first[:, lanes], second[:, lanes]]
            if fill:
                parts.append(jnp.zeros((fill, TILE), jnp.float32))
            strided[pl.ds(t * TILE, TILE), :] = jnp.concatenate(parts, axis=0).T
        for k in range(self.outer):
            slab = strided[pl.ds(k, self.inner, stride=self.outer), :].T
            result[k] = slab[: 2 * rows, :]

    def collect(self, slabs, strided, results):
        rows = self.rows
        for k in range(self.outer):
            slab = slabs(k)
            fill = TILE - slab.shape[0]
            if fill:
                slab = jnp.concatenate([slab, jnp.zeros((fill, self.inner), jnp.float32)], axis=0)
            strided[pl.ds(k, self.inner, stride=self.outer), :] = slab.T
        for t in range(self.length // TILE):
            block = strided[pl.ds(t * TILE, TILE), :].T
            for i, result in enumerate(results):
                result[:, pl.ds(t * TILE, TILE)] = block[i * rows : (i + 1) * rows, :]


def signed_waves(position, count):
    signed = jnp.where(position < count // 2, position, position - count)
    waves = 4.0 * signed.astype(jnp.float32) / count
    return waves, jnp.where(position == count // 2, jnp.float32(0.0), waves)


def first_waves(piece, k):
    lanes = lax.broadcasted_iota(jnp.int32, (1, piece.inner), 1)
    return signed_waves(piece.outer * lanes + k, piece.length)


def inverse_denominator(wave_first, wave_second):
    square = wave_first * wave_first + wave_second * wave_second
    return 1.0 / (1.0 + time_step * (square * square - square))


def second_wave(piece, position):
    shape = (position.shape[0], piece.inner)
    return jnp.broadcast_to(signed_waves(position, piece.length)[0], shape)


def row_index(count, width):
    return lax.broadcasted_iota(jnp.int32, (count, width), 0)


def start_kernel(length, rows, field, target, twiddle, matrix, out, both_p, *scratch):
    piece = Pieces(length, rows, *scratch[:4])
    piece.spread(field, target, scratch[4], both_p)

    def body(r0):
        at = pl.ds(r0, piece.step)
        for k in range(piece.outer):
            piece.put(k, at, 0, both_p[k, at, :])

    piece.chunks(rows, body)
    piece.outgoing_kept(twiddle, matrix, out)


def slope_second_kernel(length, rows, field_p, twiddle, out_matrix, in_matrix, kept, result, *scratch):
    piece = Pieces(length, rows, *scratch)

    def body(r0):
        at = pl.ds(r0, piece.step)
        for k in range(piece.outer):
            piece.put(k, at, 0, field_p[k, at, :])

    piece.chunks(rows, body)
    for j in range(piece.outer):
        piece.clear_other(j)

    def write(r0, items):
        for j, (re, im) in enumerate(items):
            at, wide = piece.kept_lanes(j)
            base = at - j * piece.inner
            position = j * piece.inner + kept[:, base : base + wide]
            slope = 2.0 * signed_waves(position, length)[1]
            piece.turned[pl.ds(r0, piece.step), pl.ds(at, wide)] = -slope * im[:, base : base + wide]
            piece.turned[pl.ds(rows + r0, piece.step), pl.ds(at, wide)] = slope * re[:, base : base + wide]

    piece.outgoing(rows, -1.0, twiddle, out_matrix, True, write)
    piece.incoming(rows, 1.0, twiddle, in_matrix, real_out=True)
    result[...] = piece.z[:, :, : piece.inner]


def spread_kernel(length, rows, forcing, result, strided):
    Pieces(length, rows).spread(forcing.at[0], forcing.at[1], strided, result)


def collect_kernel(length, rows, slabs, result, strided):
    piece = Pieces(length, rows)
    piece.collect(lambda k: slabs[k], strided, [result.at[i] for i in range(result.shape[0])])


def weight_of(device, r0, step, inner):
    alone = (row_index(step, inner) + r0 + device) == 0
    return jnp.where(alone, jnp.float32(1.0), jnp.float32(2.0))


def slope_kernel(length, rows, device_ref, source, in_twiddle, in_matrix, out_twiddle, out_matrix, out, state, *scratch):
    device = device_ref[0]
    piece = Pieces(length, rows, *scratch)
    half = piece.half
    piece.turn_lines(source)
    piece.incoming(half, -1.0, in_twiddle, in_matrix)

    def body(r0):
        at, also = pl.ds(r0, piece.step), pl.ds(half + r0, piece.step)
        weight = weight_of(device, r0, piece.step, piece.inner)
        for k in range(piece.outer):
            re, im = piece.get(k, at, 0), piece.get(k, at, 1)
            state[k, at, :], state[k, also, :] = re, im
            scale = first_waves(piece, k)[1] * weight
            piece.put(k, at, 0, -scale * im)
            piece.put(k, at, 1, scale * re)

    piece.chunks(half, body)
    piece.outgoing(half, 1.0, out_twiddle, out_matrix, False, piece.write_full(out, False))


def total_kernel(length, rows, device_ref, source, coef, in_twiddle, in_matrix, out_twiddle, out_matrix, out, *scratch):
    device = device_ref[0]
    piece = Pieces(length, rows, *scratch)
    half = piece.half
    piece.turn_lines(source)
    piece.incoming(half, -1.0, in_twiddle, in_matrix)

    def body(r0):
        at, also = pl.ds(r0, piece.step), pl.ds(half + r0, piece.step)
        weight = weight_of(device, r0, piece.step, piece.inner)
        for k in range(piece.outer):
            re, im = piece.get(k, at, 0), piece.get(k, at, 1)
            deriv = first_waves(piece, k)[1]
            scale = 1.0 / time_step
            piece.put(k, at, 0, weight * (scale * coef[k, at, :] - deriv * im))
            piece.put(k, at, 1, weight * (scale * coef[k, also, :] + deriv * re))

    piece.chunks(half, body)
    piece.outgoing(half, 1.0, out_twiddle, out_matrix, False, piece.write_full(out, False))


def edge_inverses(piece, k):
    wave_first = first_waves(piece, k)[0]
    middle = jnp.full((1, 1), piece.length // 2, jnp.int32)
    zero = jnp.zeros((1, 1), jnp.int32)
    return [inverse_denominator(wave_first, signed_waves(p, piece.length)[0]) for p in (zero, middle)]


def next_kernel(length, rows, device_ref, source, state, forcing, in_twiddle, in_matrix, out_twiddle, out_matrix, mirror, out, *scratch):
    device = device_ref[0]
    piece = Pieces(length, rows, *scratch)
    half, step, inner = piece.half, piece.step, piece.inner
    late = device >= (length // rows) // 2
    piece.turn_lines(source)
    piece.incoming(half, -1.0, in_twiddle, in_matrix)

    def body(r0):
        at, also = pl.ds(r0, step), pl.ds(half + r0, step)
        index = row_index(step, 1) + r0
        low_wave = second_wave(piece, device * rows + index)
        high_wave = second_wave(piece, device * rows + half + index)
        moved = jnp.logical_and(row_index(step, inner) + r0 == 0, late)
        weight = weight_of(device, r0, step, inner)
        for k in range(piece.outer):
            wave_first = first_waves(piece, k)[0]
            low = inverse_denominator(wave_first, low_wave)
            high = inverse_denominator(wave_first, high_wave)
            for part in range(2):
                own = state[k, pl.ds(part * half + r0, step), :] + time_step * piece.get(k, at, part)
                own = weight * own
                f_low = time_step * forcing[k, pl.ds(part * rows + r0, step), :]
                f_high = time_step * forcing[k, pl.ds(part * rows + half + r0, step), :]
                piece.put(k, at, part, (f_low + jnp.where(moved, 0.0, own)) * low)
                piece.put(k, also, part, (f_high + jnp.where(moved, own, 0.0)) * high)

    piece.chunks(half, body)

    @pl.when(device == 0)
    def _():
        at = pl.ds(0, 8)
        blocks = []
        for k in range(piece.outer):
            own = tuple(
                state[k, pl.ds(part * half, 8), :] + time_step * piece.get(k, at, part) for part in range(2)
            )
            full = tuple(
                own[part] + time_step * forcing[k, pl.ds(part * rows, 8), :] for part in range(2)
            )
            blocks.append([own, full])
        flipped = piece.mirrored(blocks, mirror)
        rest = pl.ds(0, 16)
        row0 = row_index(16, inner) == 0
        for k in range(piece.outer):
            zero, middle = edge_inverses(piece, k)
            for part in range(2):
                own, full = blocks[k][0][part], blocks[k][1][part]
                own_c, full_c = flipped[k][0][part], flipped[k][1][part]
                value = 0.5 * ((full + full_c) * zero + (own - own_c) * middle)
                replace(piece, k, part, value)

    piece.outgoing(rows, 1.0, out_twiddle, out_matrix, False, piece.write_full(out, False))


def replace(piece, k, part, value):
    lanes = pl.ds(part * piece.inner, piece.inner)
    row0 = row_index(16, piece.inner) == 0
    value = jnp.concatenate([value, value], axis=0)
    for held, new in zip((piece.top, piece.low), halves(value)):
        old = held[k, pl.ds(0, 16), lanes].astype(jnp.float32)
        held[k, pl.ds(0, 16), lanes] = jnp.where(row0, new.astype(jnp.float32), old).astype(jnp.bfloat16)


def misfit_kernel(length, rows, device_ref, source, in_twiddle, in_matrix, out_twiddle, out_matrix, mirror, out, full, coef, total_out, *scratch):
    device = device_ref[0]
    piece = Pieces(length, rows, *scratch)
    half, step, inner = piece.half, piece.step, piece.inner
    late = device >= (length // rows) // 2
    piece.turn_full(source)
    piece.incoming(rows, -1.0, in_twiddle, in_matrix)

    def body(r0):
        at, also = pl.ds(r0, step), pl.ds(half + r0, step)
        index = row_index(step, 1) + r0
        low_wave = second_wave(piece, device * rows + index)
        high_wave = second_wave(piece, device * rows + half + index)
        moved = jnp.logical_and(row_index(step, inner) + r0 == 0, late)
        weight = weight_of(device, r0, step, inner)
        for k in range(piece.outer):
            wave_first = first_waves(piece, k)[0]
            low = time_step * inverse_denominator(wave_first, low_wave)
            high = time_step * inverse_denominator(wave_first, high_wave)
            for part in range(2):
                low_value = piece.get(k, at, part) * low
                high_value = piece.get(k, also, part) * high
                full[k, pl.ds(part * rows + r0, step), :] = low_value
                full[k, pl.ds(part * rows + half + r0, step), :] = high_value
                own = jnp.where(moved, high_value, low_value)
                coef[k, pl.ds(part * half + r0, step), :] = own
                piece.put(k, at, part, weight * own)

    piece.chunks(half, body)

    @pl.when(device == 0)
    def _():
        at = pl.ds(0, 8)
        blocks = [[(piece.get(k, at, 0), piece.get(k, at, 1))] for k in range(piece.outer)]
        flipped = piece.mirrored(blocks, mirror)
        row0 = row_index(8, inner) == 0
        for k in range(piece.outer):
            zero, middle = edge_inverses(piece, k)
            for part in range(2):
                own, own_c = blocks[k][0][part], flipped[k][0][part]
                first = (0.5 * time_step) * (own + own_c) * zero
                value = first + (0.5 * time_step) * (own - own_c) * middle
                at_full, at_coef = pl.ds(part * rows, 8), pl.ds(part * half, 8)
                full[k, at_full, :] = jnp.where(row0, first, full[k, at_full, :])
                coef[k, at_coef, :] = jnp.where(row0, value, coef[k, at_coef, :])
                replace(piece, k, part, value)

    piece.outgoing(half, 1.0, out_twiddle, out_matrix, False, piece.write_full(out, False))
    total_out[...] = jnp.sum(source[:, pl.ds(rows, 8), :], axis=0)


def nonlinear_kernel(length, rows, source, second, twiddle, in_matrix, out_matrix, out, first_out, *scratch):
    piece = Pieces(length, rows, *scratch)
    piece.turn_kept(source)
    piece.unpack_middle()
    piece.incoming(rows, 1.0, twiddle, in_matrix, real_out=True)

    def body(r0):
        at = pl.ds(r0, piece.step)
        for k in range(piece.outer):
            first, other = piece.get(k, at, 0), second[k, at, :]
            first_out[k, at, :] = first
            piece.put(k, at, 0, -0.5 * (first * first + other * other))

    piece.chunks(rows, body)
    piece.outgoing_kept(twiddle, out_matrix, out)


def joint_kernel(length, rows, source, first, second, twiddle, in_matrix, out_matrix, out, second_out, *scratch):
    piece = Pieces(length, rows, *scratch)
    piece.turn_kept(source)
    piece.unpack_middle()
    piece.incoming(rows, 1.0, twiddle, in_matrix, real_out=True)

    def body(r0):
        at = pl.ds(r0, piece.step)
        for k in range(piece.outer):
            value = piece.get(k, at, 0)
            second_out[k, at, :] = value * second[k, at, :]
            piece.put(k, at, 0, value * first[k, at, :])

    piece.chunks(rows, body)
    piece.outgoing_kept(twiddle, out_matrix, out)


def residual_kernel(length, rows, source, both_p, twiddle, in_matrix, out_matrix, out, field_out, *scratch):
    piece = Pieces(length, rows, *scratch[:4])
    strided, total = scratch[4:]
    piece.turn_full(source)
    piece.unpack_middle()
    piece.incoming(rows, 1.0, twiddle, in_matrix, real_out=True)
    piece.collect(lambda k: piece.get(k, pl.ds(0, rows), 0), strided, [field_out])
    total[...] = jnp.zeros_like(total)

    def body(r0):
        at = pl.ds(r0, piece.step)
        for k in range(piece.outer):
            residual = piece.get(k, at, 0) - both_p[k, pl.ds(rows + r0, piece.step), :]
            total[...] += residual * residual
            piece.put(k, at, 0, residual)

    piece.chunks(rows, body)
    piece.outgoing(rows, -1.0, twiddle, out_matrix, True, piece.write_full(out, True))
    value = 0.5 * jnp.sum(total[...])
    out[:, pl.ds(rows, 8), :] = jnp.full((out.shape[0], 8, 2 * rows), value, jnp.float32)


def last_kernel(length, rows, source, second, twiddle, in_matrix, field_out, *scratch):
    piece = Pieces(length, rows, *scratch[:4])
    piece.turn_kept(source)
    piece.unpack_middle()
    piece.incoming(rows, 1.0, twiddle, in_matrix, real_out=True)
    piece.collect(
        lambda k: piece.get(k, pl.ds(0, rows), 0) + second[k], scratch[4], [field_out]
    )


def member_step(device, field, target, forcing_p, devices, rows, length):
    outer, inner = split_length(length)
    half = rows // 2
    float32 = jnp.float32
    shape = lambda *dims: jax.ShapeDtypeStruct(dims, float32)
    kept_blocks = shape(devices, rows * rows // TILE, TILE)
    half_blocks = shape(devices, half, 2 * rows)
    blocks = shape(devices, rows, 2 * rows)
    longer = shape(devices, rows + 8, 2 * rows)
    pair, one = shape(outer, 2 * rows, inner), shape(outer, rows, inner)
    plain = shape(rows, length)
    step = math.gcd(half, 16)
    base = [
        pltpu.VMEM((2 * rows, length), float32),
        pltpu.VMEM((outer, rows, 2 * inner), jnp.bfloat16),
        pltpu.VMEM((outer, rows, 2 * inner), jnp.bfloat16),
        pltpu.VMEM((outer, rows, 2 * inner), float32),
    ]
    strided = pltpu.VMEM((length, TILE), float32)
    total = pltpu.VMEM((step, inner), float32)
    vmem = pl.BlockSpec(memory_space=pltpu.VMEM)
    smem = pl.BlockSpec(memory_space=pltpu.SMEM)

    natural, kept, lines = orders(length, rows)
    tw_natural, tw_kept, tw_lines = [jnp.asarray(twiddle_table(length, o)) for o in (natural, kept, lines)]
    matrix = lambda *args: matrix_table(length, *args)
    forward, backward = matrix(-1.0, natural, natural), matrix(1.0, natural, natural)
    kept_out, kept_in = matrix(-1.0, natural, kept)[:, :inner], matrix(1.0, kept, natural)[:, :, :inner]
    lines_in = matrix(-1.0, lines, natural)
    mirror = jnp.asarray(mirror_table(length))
    kept_lane = jnp.asarray(kept[None, :].astype(np.int32))

    def call(body, outs, scratch, *operands):
        return pl.pallas_call(
            functools.partial(body, length, rows),
            out_shape=outs,
            in_specs=[smem if operand is device else vmem for operand in operands],
            out_specs=jax.tree.map(lambda leaf: vmem, outs),
            scratch_shapes=scratch,
            compiler_params=pltpu.CompilerParams(vmem_limit_bytes=20 * 2**20),
            cost_estimate=pl.CostEstimate(flops=6 * 10**9, bytes_accessed=4 * 2**20, transcendentals=0),
        )(*operands)

    def move(value):
        return lax.all_to_all(value, axes, split_axis=0, concat_axis=0, tiled=True)

    spectral_tables = (tw_lines, lines_in, tw_natural, backward)
    slope_tables = (tw_kept, kept_out, kept_in, kept_lane)
    sent, both_p = call(start_kernel, (kept_blocks, pair), base + [strided], field, target, tw_kept, kept_out)
    second = call(slope_second_kernel, one, base, both_p, *slope_tables)
    sent, state = call(slope_kernel, (half_blocks, one), base, device, move(sent), *spectral_tables)
    sent, first = call(nonlinear_kernel, (kept_blocks, one), base, move(sent), second, tw_kept, kept_in, kept_out)
    sent = call(next_kernel, blocks, base, device, move(sent), state, forcing_p, *spectral_tables, mirror)
    sent, next_field = call(
        residual_kernel, (longer, plain), base + [strided, total],
        move(sent), both_p, tw_natural, backward, forward,
    )
    sent, full, coef, sums = call(
        misfit_kernel, (half_blocks, pair, one, shape(8, 2 * rows)), base,
        device, move(sent), tw_natural, forward, tw_natural, backward, mirror,
    )
    sent, product = call(
        joint_kernel, (kept_blocks, one), base, move(sent), first, second, tw_kept, kept_in, kept_out
    )
    second_part = call(slope_second_kernel, one, base, product, *slope_tables)
    sent = call(total_kernel, half_blocks, base, device, move(sent), coef, *spectral_tables)
    field_grad = call(last_kernel, plain, base + [strided], move(sent), second_part, tw_kept, kept_in)
    return next_field, sums[0, 0], field_grad, full


def per_device(devices, initial_field, target_field, forcing):
    members, rows, length = initial_field.shape
    device = lax.axis_index(axes).astype(jnp.int32).reshape(1)
    outer, inner = split_length(length)
    vmem = pl.BlockSpec(memory_space=pltpu.VMEM)
    strided = pltpu.VMEM((length, TILE), jnp.float32)

    def reorder(body, shape, operand):
        return pl.pallas_call(
            functools.partial(body, length, rows),
            out_shape=jax.ShapeDtypeStruct(shape, jnp.float32),
            in_specs=[vmem],
            out_specs=vmem,
            scratch_shapes=[strided],
        )(operand)

    forcing_p = reorder(spread_kernel, (outer, 2 * rows, inner), forcing)
    results = [
        member_step(device, initial_field[m], target_field[m], forcing_p, devices, rows, length)
        for m in range(members)
    ]
    next_field = jnp.stack([one[0] for one in results])
    objective = sum(one[1] for one in results) / (members * length * length)
    field_grad = jnp.stack([one[2] for one in results])
    forcing_grad = reorder(collect_kernel, (2, rows, length), sum(one[3] for one in results))
    return (next_field, objective, field_grad, forcing_grad)


def solution(mesh):
    devices = mesh.shape["px"] * mesh.shape["py"]
    spec = P(None, axes, None)
    return jax.shard_map(
        functools.partial(per_device, devices),
        mesh=mesh,
        in_specs=(spec, spec, spec),
        out_specs=(spec, P(), spec, spec),
        check_vma=False,
    )
```

```python
import functools
import math

import jax
import jax.numpy as jnp
import numpy as np
from jax import lax
from jax.experimental import pallas as pl
from jax.experimental.pallas import tpu as pltpu
from jax.sharding import PartitionSpec as P

time_step = 0.25
axes = ("px", "py")
TILE = 128


def split_length(length):
    inner = 256 if length % 256 == 0 else TILE
    return (length // inner, inner)


def small_dft(items, sign):
    count = len(items)
    if count == 1:
        return items
    evens = small_dft(items[0::2], sign)
    odds = small_dft(items[1::2], sign)
    low, high = [], []
    for k in range(count // 2):
        odd_re, odd_im = odds[k]
        if 4 * k == count:
            odd_re, odd_im = (-odd_im, odd_re) if sign > 0 else (odd_im, -odd_re)
        elif k:
            c = math.cos(2.0 * math.pi * k / count)
            s = sign * math.sin(2.0 * math.pi * k / count)
            if abs(abs(c) - abs(s)) < 1e-12:
                sc, ss = math.copysign(1.0, c), math.copysign(1.0, s)
                odd_re, odd_im = (
                    c * (odd_re - sc * ss * odd_im),
                    c * (odd_im + sc * ss * odd_re),
                )
            else:
                odd_re, odd_im = (c * odd_re - s * odd_im, c * odd_im + s * odd_re)
        even_re, even_im = evens[k]
        low.append((even_re + odd_re, even_im + odd_im))
        high.append((even_re - odd_re, even_im - odd_im))
    return low + high


def halves(value):
    top = value.astype(jnp.bfloat16)
    return top, (value - top.astype(jnp.float32)).astype(jnp.bfloat16)


def orders(length, rows):
    inner = split_length(length)[1]
    half = rows // 2
    lane = np.arange(inner)
    natural = lane
    local = lane % (inner // 2)
    line = local % half
    kept = rows * (local // half) + np.where((lane >= inner // 2) & (line == 0), half, line)
    groups = TILE // rows
    tall = rows // groups
    within = lane % (inner // groups)
    lines = rows * (within // tall) + tall * (lane // (inner // groups)) + within % tall
    return natural, kept, lines


def twiddle_table(length, order):
    outer = split_length(length)[0]
    angle = 2.0 * np.pi * np.outer(np.arange(outer), order) / length
    return (np.stack([np.cos(angle), np.sin(angle)]) / math.sqrt(length)).astype(np.float32)


def matrix_table(length, sign, left, right):
    inner = split_length(length)[1]
    angle = 2.0 * np.pi * (np.outer(left, right) % inner) / inner
    c, s = np.cos(angle), np.sin(angle)
    full = np.block([[c, sign * s], [-sign * s, c]])
    top = full.astype(jnp.bfloat16)
    return np.stack([top, (full - top.astype(np.float64)).astype(jnp.bfloat16)])


def mirror_table(length):
    inner = split_length(length)[1]
    lane = np.arange(inner)
    both = np.zeros((2, inner, inner))
    both[0, (inner - lane) % inner, lane] = 1.0
    both[1, inner - 1 - lane, lane] = 1.0
    return both.astype(jnp.bfloat16)


class Pieces:
    def __init__(self, length, rows, turned=None, top=None, low=None, grid_out=None):
        self.length, self.rows, self.half = length, rows, rows // 2
        self.outer, self.inner = split_length(length)
        self.turned, self.top, self.low, self.z = turned, top, low, grid_out
        self.step = math.gcd(rows // 2, 16)

    def chunks(self, lines, body):
        def run(i, carry):
            body(pl.multiple_of(i * self.step, self.step))
            return carry

        lax.fori_loop(0, lines // self.step, run, 0)

    def put(self, k, at, part, value):
        lanes = pl.ds(part * self.inner, self.inner)
        top, low = halves(value)
        self.top[k, at, lanes] = top
        self.low[k, at, lanes] = low

    def get(self, k, at, part):
        return self.z[k, at, pl.ds(part * self.inner, self.inner)]

    def multiply(self, lines, matrix, real_in=False, real_out=False):
        deep = self.inner if real_in else 2 * self.inner
        wide = self.inner if real_out else 2 * self.inner
        count = self.outer * lines
        top = self.top[:, :lines, :deep].reshape(count, deep)
        low = self.low[:, :lines, :deep].reshape(count, deep)
        right_top = matrix[0, :deep, :wide]
        right_low = matrix[1, :deep, :wide]
        dot = functools.partial(jnp.dot, preferred_element_type=jnp.float32)
        total = dot(top, right_top) + dot(low, right_top) + dot(top, right_low)
        self.z[:, :lines, :wide] = total.reshape(self.outer, lines, wide)

    def twist(self, k, pair, sign, twiddle):
        c = twiddle[0, pl.ds(k, 1), :]
        s = twiddle[1, pl.ds(k, 1), :]
        s = s if sign > 0 else -s
        re, im = pair
        return (re * c - im * s, re * s + im * c)

    def turn_full(self, source):
        rows, blocks = self.rows, TILE // self.rows
        for t in range(self.length // TILE):
            tile = source[pl.ds(t * blocks, blocks), :rows, :].reshape(TILE, 2 * rows)
            self.turned[: 2 * rows, pl.ds(t * TILE, TILE)] = tile.T

    def turn_lines(self, source):
        rows = self.rows
        groups = TILE // rows
        blocks, wide = self.inner // rows, self.inner // groups
        for t in range(self.outer):
            tile = source[pl.ds(t * blocks, blocks), :, :].reshape(wide, TILE).T
            for h in range(groups):
                self.turned[:rows, pl.ds(t * self.inner + h * wide, wide)] = tile[h * rows : (h + 1) * rows]

    def kept_lanes(self, j):
        wide = self.inner // 2
        return j * self.inner + (wide if 2 * j >= self.outer else 0), wide

    def clear_other(self, j):
        at, wide = self.kept_lanes(j)
        other = j * self.inner + (0 if 2 * j >= self.outer else wide)
        self.turned[: 2 * self.rows, pl.ds(other, wide)] = jnp.zeros((2 * self.rows, wide), jnp.float32)

    def turn_kept(self, source):
        rows, half, blocks = self.rows, self.half, self.inner // self.rows
        for j in range(self.outer):
            at, wide = self.kept_lanes(j)
            tile = source[pl.ds(j * blocks, blocks), :, :].reshape(wide, 2 * rows)
            self.turned[: 2 * rows, pl.ds(at, wide)] = tile.T
            self.clear_other(j)

    def unpack_middle(self):
        rows, middle = self.rows, (self.outer // 2) * self.inner
        first = self.turned[rows : 2 * rows, :TILE]
        lane0 = lax.broadcasted_iota(jnp.int32, first.shape, 1) == 0
        zero = jnp.zeros_like(first)
        self.turned[:rows, pl.ds(middle, TILE)] += jnp.where(lane0, first, zero)
        self.turned[rows : 2 * rows, :TILE] = jnp.where(lane0, zero, first)

    def incoming(self, lines, sign, twiddle, matrix, real_out=False):
        def body(r0):
            items = []
            for j in range(self.outer):
                lanes = pl.ds(j * self.inner, self.inner)
                items.append((
                    self.turned[pl.ds(r0, self.step), lanes],
                    self.turned[pl.ds(lines + r0, self.step), lanes],
                ))
            for k, pair in enumerate(small_dft(items, sign)):
                re, im = self.twist(k, pair, sign, twiddle)
                self.put(k, pl.ds(r0, self.step), 0, re)
                self.put(k, pl.ds(r0, self.step), 1, im)

        self.chunks(lines, body)
        self.multiply(lines, matrix, real_out=real_out)

    def outgoing(self, lines, sign, twiddle, matrix, real_in, write):
        self.multiply(lines, matrix, real_in=real_in)

        def body(r0):
            at = pl.ds(r0, self.step)
            write(r0, small_dft([
                self.twist(k, (self.get(k, at, 0), self.get(k, at, 1)), sign, twiddle)
                for k in range(self.outer)
            ], sign))

        self.chunks(lines, body)

    def pack_middle(self, items):
        re, im = items[0]
        lane0 = lax.broadcasted_iota(jnp.int32, im.shape, 1) == 0
        return [(re, jnp.where(lane0, items[self.outer // 2][0], im))] + items[1:]

    def write_full(self, result, pack):
        rows = self.rows

        def write(r0, items):
            at = pl.ds(r0, self.step)
            for j, (re, im) in enumerate(self.pack_middle(items) if pack else items):
                for piece in range(self.inner // rows):
                    to = j * (self.inner // rows) + piece
                    lanes = slice(piece * rows, (piece + 1) * rows)
                    result[to, at, pl.ds(0, rows)] = re[:, lanes]
                    result[to, at, pl.ds(rows, rows)] = im[:, lanes]

        return write

    def outgoing_kept(self, twiddle, matrix, result):
        self.multiply(self.rows, matrix, real_in=True)
        rows, half, blocks = self.rows, self.half, self.inner // self.rows
        tall = rows * rows // TILE
        step = math.gcd(rows, 16)
        span = min(tall, step)
        for h in range(rows // max(tall, step)):

            def body(i, carry, h=h):
                r0 = i * step if isinstance(i, int) else pl.multiple_of(i * step, step)
                at = pl.ds(h * max(tall, step) + r0, step)
                items = self.pack_middle(small_dft([
                    self.twist(k, (self.get(k, at, 0), self.get(k, at, 1)), -1.0, twiddle)
                    for k in range(self.outer)
                ], -1.0))
                for j, pair in enumerate(items):
                    base = self.inner // 2 if 2 * j >= self.outer else 0
                    for piece in range(blocks):
                        lanes = slice(base + piece * half, base + (piece + 1) * half)
                        for part, value in enumerate(pair):
                            for sub in range(step // span):
                                group = h * (step // span) + sub
                                to = pl.ds(group * rows + part * half, half)
                                held = value[sub * span : (sub + 1) * span, lanes]
                                result[j * blocks + piece, pl.ds(r0, span), to] = held
                return carry

            if tall > step:
                lax.fori_loop(0, tall // step, body, 0)
            else:
                body(0, 0)

    def mirrored(self, blocks, mirror):
        dot = functools.partial(jnp.dot, preferred_element_type=jnp.float32)

        def flip(values, which):
            top, low = halves(jnp.concatenate(values, axis=0))
            return dot(top, mirror[which]) + dot(low, mirror[which])

        flat = [part for k in range(self.outer) for pair in blocks[k] for part in pair]
        per = 2 * len(blocks[0])
        low = flip(flat[:per], 0)
        high = flip(flat[per:], 1)
        out = []
        for k in range(self.outer):
            part, base = (low, 0) if k == 0 else (high, (self.outer - k - 1) * per)
            take = lambda i: part[(base + i) * 8 : (base + i + 1) * 8]
            out.append([(take(2 * i), -take(2 * i + 1)) for i in range(per // 2)])
        return out

    def spread(self, first, second, strided, result):
        rows, fill = self.rows, TILE - 2 * self.rows
        for t in range(self.length // TILE):
            lanes = pl.ds(t * TILE, TILE)
            parts = [first[:, lanes], second[:, lanes]]
            if fill:
                parts.append(jnp.zeros((fill, TILE), jnp.float32))
            strided[pl.ds(t * TILE, TILE), :] = jnp.concatenate(parts, axis=0).T
        for k in range(self.outer):
            slab = strided[pl.ds(k, self.inner, stride=self.outer), :].T
            result[k] = slab[: 2 * rows, :]

    def collect(self, slabs, strided, results):
        rows = self.rows
        for k in range(self.outer):
            slab = slabs(k)
            fill = TILE - slab.shape[0]
            if fill:
                slab = jnp.concatenate([slab, jnp.zeros((fill, self.inner), jnp.float32)], axis=0)
            strided[pl.ds(k, self.inner, stride=self.outer), :] = slab.T
        for t in range(self.length // TILE):
            block = strided[pl.ds(t * TILE, TILE), :].T
            for i, result in enumerate(results):
                result[:, pl.ds(t * TILE, TILE)] = block[i * rows : (i + 1) * rows, :]


def signed_waves(position, count):
    signed = jnp.where(position < count // 2, position, position - count)
    waves = 4.0 * signed.astype(jnp.float32) / count
    return waves, jnp.where(position == count // 2, jnp.float32(0.0), waves)


def first_waves(piece, k):
    lanes = lax.broadcasted_iota(jnp.int32, (1, piece.inner), 1)
    return signed_waves(piece.outer * lanes + k, piece.length)


def inverse_denominator(wave_first, wave_second):
    square = wave_first * wave_first + wave_second * wave_second
    return 1.0 / (1.0 + time_step * (square * square - square))


def second_wave(piece, position):
    shape = (position.shape[0], piece.inner)
    return jnp.broadcast_to(signed_waves(position, piece.length)[0], shape)


def row_index(count, width):
    return lax.broadcasted_iota(jnp.int32, (count, width), 0)


def start_kernel(length, rows, field, target, twiddle, matrix, out, both_p, *scratch):
    piece = Pieces(length, rows, *scratch[:4])
    piece.spread(field, target, scratch[4], both_p)

    def body(r0):
        at = pl.ds(r0, piece.step)
        for k in range(piece.outer):
            piece.put(k, at, 0, both_p[k, at, :])

    piece.chunks(rows, body)
    piece.outgoing_kept(twiddle, matrix, out)


def slope_second_kernel(length, rows, field_p, twiddle, out_matrix, in_matrix, kept, result, *scratch):
    piece = Pieces(length, rows, *scratch)

    def body(r0):
        at = pl.ds(r0, piece.step)
        for k in range(piece.outer):
            piece.put(k, at, 0, field_p[k, at, :])

    piece.chunks(rows, body)
    for j in range(piece.outer):
        piece.clear_other(j)

    def write(r0, items):
        for j, (re, im) in enumerate(items):
            at, wide = piece.kept_lanes(j)
            base = at - j * piece.inner
            position = j * piece.inner + kept[:, base : base + wide]
            slope = 2.0 * signed_waves(position, length)[1]
            piece.turned[pl.ds(r0, piece.step), pl.ds(at, wide)] = -slope * im[:, base : base + wide]
            piece.turned[pl.ds(rows + r0, piece.step), pl.ds(at, wide)] = slope * re[:, base : base + wide]

    piece.outgoing(rows, -1.0, twiddle, out_matrix, True, write)
    piece.incoming(rows, 1.0, twiddle, in_matrix, real_out=True)
    result[...] = piece.z[:, :, : piece.inner]


def spread_kernel(length, rows, forcing, result, strided):
    Pieces(length, rows).spread(forcing.at[0], forcing.at[1], strided, result)


def collect_kernel(length, rows, slabs, result, strided):
    piece = Pieces(length, rows)
    piece.collect(lambda k: slabs[k], strided, [result.at[i] for i in range(result.shape[0])])


def weight_of(device, r0, step, inner):
    alone = (row_index(step, inner) + r0 + device) == 0
    return jnp.where(alone, jnp.float32(1.0), jnp.float32(2.0))


def slope_kernel(length, rows, device_ref, source, in_twiddle, in_matrix, out_twiddle, out_matrix, out, state, *scratch):
    device = device_ref[0]
    piece = Pieces(length, rows, *scratch)
    half = piece.half
    piece.turn_lines(source)
    piece.incoming(half, -1.0, in_twiddle, in_matrix)

    def body(r0):
        at, also = pl.ds(r0, piece.step), pl.ds(half + r0, piece.step)
        weight = weight_of(device, r0, piece.step, piece.inner)
        for k in range(piece.outer):
            re, im = piece.get(k, at, 0), piece.get(k, at, 1)
            state[k, at, :], state[k, also, :] = re, im
            scale = first_waves(piece, k)[1] * weight
            piece.put(k, at, 0, -scale * im)
            piece.put(k, at, 1, scale * re)

    piece.chunks(half, body)
    piece.outgoing(half, 1.0, out_twiddle, out_matrix, False, piece.write_full(out, False))


def total_kernel(length, rows, device_ref, source, coef, in_twiddle, in_matrix, out_twiddle, out_matrix, out, *scratch):
    device = device_ref[0]
    piece = Pieces(length, rows, *scratch)
    half = piece.half
    piece.turn_lines(source)
    piece.incoming(half, -1.0, in_twiddle, in_matrix)

    def body(r0):
        at, also = pl.ds(r0, piece.step), pl.ds(half + r0, piece.step)
        weight = weight_of(device, r0, piece.step, piece.inner)
        for k in range(piece.outer):
            re, im = piece.get(k, at, 0), piece.get(k, at, 1)
            deriv = first_waves(piece, k)[1]
            scale = 1.0 / time_step
            piece.put(k, at, 0, weight * (scale * coef[k, at, :] - deriv * im))
            piece.put(k, at, 1, weight * (scale * coef[k, also, :] + deriv * re))

    piece.chunks(half, body)
    piece.outgoing(half, 1.0, out_twiddle, out_matrix, False, piece.write_full(out, False))


def edge_inverses(piece, k):
    wave_first = first_waves(piece, k)[0]
    middle = jnp.full((1, 1), piece.length // 2, jnp.int32)
    zero = jnp.zeros((1, 1), jnp.int32)
    return [inverse_denominator(wave_first, signed_waves(p, piece.length)[0]) for p in (zero, middle)]


def next_kernel(length, rows, device_ref, source, state, forcing, in_twiddle, in_matrix, out_twiddle, out_matrix, mirror, out, *scratch):
    device = device_ref[0]
    piece = Pieces(length, rows, *scratch)
    half, step, inner = piece.half, piece.step, piece.inner
    late = device >= (length // rows) // 2
    piece.turn_lines(source)
    piece.incoming(half, -1.0, in_twiddle, in_matrix)

    def body(r0):
        at, also = pl.ds(r0, step), pl.ds(half + r0, step)
        index = row_index(step, 1) + r0
        low_wave = second_wave(piece, device * rows + index)
        high_wave = second_wave(piece, device * rows + half + index)
        moved = jnp.logical_and(row_index(step, inner) + r0 == 0, late)
        weight = weight_of(device, r0, step, inner)
        for k in range(piece.outer):
            wave_first = first_waves(piece, k)[0]
            low = inverse_denominator(wave_first, low_wave)
            high = inverse_denominator(wave_first, high_wave)
            for part in range(2):
                own = state[k, pl.ds(part * half + r0, step), :] + time_step * piece.get(k, at, part)
                own = weight * own
                f_low = time_step * forcing[k, pl.ds(part * rows + r0, step), :]
                f_high = time_step * forcing[k, pl.ds(part * rows + half + r0, step), :]
                piece.put(k, at, part, (f_low + jnp.where(moved, 0.0, own)) * low)
                piece.put(k, also, part, (f_high + jnp.where(moved, own, 0.0)) * high)

    piece.chunks(half, body)

    @pl.when(device == 0)
    def _():
        at = pl.ds(0, 8)
        blocks = []
        for k in range(piece.outer):
            own = tuple(
                state[k, pl.ds(part * half, 8), :] + time_step * piece.get(k, at, part) for part in range(2)
            )
            full = tuple(
                own[part] + time_step * forcing[k, pl.ds(part * rows, 8), :] for part in range(2)
            )
            blocks.append([own, full])
        flipped = piece.mirrored(blocks, mirror)
        rest = pl.ds(0, 16)
        row0 = row_index(16, inner) == 0
        for k in range(piece.outer):
            zero, middle = edge_inverses(piece, k)
            for part in range(2):
                own, full = blocks[k][0][part], blocks[k][1][part]
                own_c, full_c = flipped[k][0][part], flipped[k][1][part]
                value = 0.5 * ((full + full_c) * zero + (own - own_c) * middle)
                replace(piece, k, part, value)

    piece.outgoing(rows, 1.0, out_twiddle, out_matrix, False, piece.write_full(out, False))


def replace(piece, k, part, value):
    lanes = pl.ds(part * piece.inner, piece.inner)
    row0 = row_index(16, piece.inner) == 0
    value = jnp.concatenate([value, value], axis=0)
    for held, new in zip((piece.top, piece.low), halves(value)):
        old = held[k, pl.ds(0, 16), lanes].astype(jnp.float32)
        held[k, pl.ds(0, 16), lanes] = jnp.where(row0, new.astype(jnp.float32), old).astype(jnp.bfloat16)


def misfit_kernel(length, rows, device_ref, source, in_twiddle, in_matrix, out_twiddle, out_matrix, mirror, out, full, coef, total_out, *scratch):
    device = device_ref[0]
    piece = Pieces(length, rows, *scratch)
    half, step, inner = piece.half, piece.step, piece.inner
    late = device >= (length // rows) // 2
    piece.turn_full(source)
    piece.incoming(rows, -1.0, in_twiddle, in_matrix)

    def body(r0):
        at, also = pl.ds(r0, step), pl.ds(half + r0, step)
        index = row_index(step, 1) + r0
        low_wave = second_wave(piece, device * rows + index)
        high_wave = second_wave(piece, device * rows + half + index)
        moved = jnp.logical_and(row_index(step, inner) + r0 == 0, late)
        weight = weight_of(device, r0, step, inner)
        for k in range(piece.outer):
            wave_first = first_waves(piece, k)[0]
            low = time_step * inverse_denominator(wave_first, low_wave)
            high = time_step * inverse_denominator(wave_first, high_wave)
            for part in range(2):
                low_value = piece.get(k, at, part) * low
                high_value = piece.get(k, also, part) * high
                full[k, pl.ds(part * rows + r0, step), :] = low_value
                full[k, pl.ds(part * rows + half + r0, step), :] = high_value
                own = jnp.where(moved, high_value, low_value)
                coef[k, pl.ds(part * half + r0, step), :] = own
                piece.put(k, at, part, weight * own)

    piece.chunks(half, body)

    @pl.when(device == 0)
    def _():
        at = pl.ds(0, 8)
        blocks = [[(piece.get(k, at, 0), piece.get(k, at, 1))] for k in range(piece.outer)]
        flipped = piece.mirrored(blocks, mirror)
        row0 = row_index(8, inner) == 0
        for k in range(piece.outer):
            zero, middle = edge_inverses(piece, k)
            for part in range(2):
                own, own_c = blocks[k][0][part], flipped[k][0][part]
                first = (0.5 * time_step) * (own + own_c) * zero
                value = first + (0.5 * time_step) * (own - own_c) * middle
                at_full, at_coef = pl.ds(part * rows, 8), pl.ds(part * half, 8)
                full[k, at_full, :] = jnp.where(row0, first, full[k, at_full, :])
                coef[k, at_coef, :] = jnp.where(row0, value, coef[k, at_coef, :])
                replace(piece, k, part, value)

    piece.outgoing(half, 1.0, out_twiddle, out_matrix, False, piece.write_full(out, False))
    total_out[...] = jnp.sum(source[:, pl.ds(rows, 8), :], axis=0)


def nonlinear_kernel(length, rows, source, second, twiddle, in_matrix, out_matrix, out, first_out, *scratch):
    piece = Pieces(length, rows, *scratch)
    piece.turn_kept(source)
    piece.unpack_middle()
    piece.incoming(rows, 1.0, twiddle, in_matrix, real_out=True)

    def body(r0):
        at = pl.ds(r0, piece.step)
        for k in range(piece.outer):
            first, other = piece.get(k, at, 0), second[k, at, :]
            first_out[k, at, :] = first
            piece.put(k, at, 0, -0.5 * (first * first + other * other))

    piece.chunks(rows, body)
    piece.outgoing_kept(twiddle, out_matrix, out)


def joint_kernel(length, rows, source, first, second, twiddle, in_matrix, out_matrix, out, second_out, *scratch):
    piece = Pieces(length, rows, *scratch)
    piece.turn_kept(source)
    piece.unpack_middle()
    piece.incoming(rows, 1.0, twiddle, in_matrix, real_out=True)

    def body(r0):
        at = pl.ds(r0, piece.step)
        for k in range(piece.outer):
            value = piece.get(k, at, 0)
            second_out[k, at, :] = value * second[k, at, :]
            piece.put(k, at, 0, value * first[k, at, :])

    piece.chunks(rows, body)
    piece.outgoing_kept(twiddle, out_matrix, out)


def residual_kernel(length, rows, source, both_p, twiddle, in_matrix, out_matrix, out, field_out, *scratch):
    piece = Pieces(length, rows, *scratch[:4])
    strided, total = scratch[4:]
    piece.turn_full(source)
    piece.unpack_middle()
    piece.incoming(rows, 1.0, twiddle, in_matrix, real_out=True)
    piece.collect(lambda k: piece.get(k, pl.ds(0, rows), 0), strided, [field_out])
    total[...] = jnp.zeros_like(total)

    def body(r0):
        at = pl.ds(r0, piece.step)
        for k in range(piece.outer):
            residual = piece.get(k, at, 0) - both_p[k, pl.ds(rows + r0, piece.step), :]
            total[...] += residual * residual
            piece.put(k, at, 0, residual)

    piece.chunks(rows, body)
    piece.outgoing(rows, -1.0, twiddle, out_matrix, True, piece.write_full(out, True))
    value = 0.5 * jnp.sum(total[...])
    out[:, pl.ds(rows, 8), :] = jnp.full((out.shape[0], 8, 2 * rows), value, jnp.float32)


def last_kernel(length, rows, source, second, twiddle, in_matrix, field_out, *scratch):
    piece = Pieces(length, rows, *scratch[:4])
    piece.turn_kept(source)
    piece.unpack_middle()
    piece.incoming(rows, 1.0, twiddle, in_matrix, real_out=True)
    piece.collect(
        lambda k: piece.get(k, pl.ds(0, rows), 0) + second[k], scratch[4], [field_out]
    )


def member_step(device, field, target, forcing_p, devices, rows, length):
    outer, inner = split_length(length)
    half = rows // 2
    float32 = jnp.float32
    shape = lambda *dims: jax.ShapeDtypeStruct(dims, float32)
    kept_blocks = shape(devices, rows * rows // TILE, TILE)
    half_blocks = shape(devices, half, 2 * rows)
    blocks = shape(devices, rows, 2 * rows)
    longer = shape(devices, rows + 8, 2 * rows)
    pair, one = shape(outer, 2 * rows, inner), shape(outer, rows, inner)
    plain = shape(rows, length)
    step = math.gcd(half, 16)
    base = [
        pltpu.VMEM((2 * rows, length), float32),
        pltpu.VMEM((outer, rows, 2 * inner), jnp.bfloat16),
        pltpu.VMEM((outer, rows, 2 * inner), jnp.bfloat16),
        pltpu.VMEM((outer, rows, 2 * inner), float32),
    ]
    strided = pltpu.VMEM((length, TILE), float32)
    total = pltpu.VMEM((step, inner), float32)
    vmem = pl.BlockSpec(memory_space=pltpu.VMEM)
    smem = pl.BlockSpec(memory_space=pltpu.SMEM)

    natural, kept, lines = orders(length, rows)
    tw_natural, tw_kept, tw_lines = [jnp.asarray(twiddle_table(length, o)) for o in (natural, kept, lines)]
    matrix = lambda *args: matrix_table(length, *args)
    forward, backward = matrix(-1.0, natural, natural), matrix(1.0, natural, natural)
    kept_out, kept_in = matrix(-1.0, natural, kept)[:, :inner], matrix(1.0, kept, natural)[:, :, :inner]
    lines_in = matrix(-1.0, lines, natural)
    mirror = jnp.asarray(mirror_table(length))
    kept_lane = jnp.asarray(kept[None, :].astype(np.int32))

    def call(body, outs, scratch, *operands):
        return pl.pallas_call(
            functools.partial(body, length, rows),
            out_shape=outs,
            in_specs=[smem if operand is device else vmem for operand in operands],
            out_specs=jax.tree.map(lambda leaf: vmem, outs),
            scratch_shapes=scratch,
            compiler_params=pltpu.CompilerParams(vmem_limit_bytes=12 * 2**20),
            cost_estimate=pl.CostEstimate(flops=6 * 10**9, bytes_accessed=4 * 2**20, transcendentals=0),
        )(*operands)

    def move(value):
        return lax.all_to_all(value, axes, split_axis=0, concat_axis=0, tiled=True)

    spectral_tables = (tw_lines, lines_in, tw_natural, backward)
    slope_tables = (tw_kept, kept_out, kept_in, kept_lane)
    sent, both_p = call(start_kernel, (kept_blocks, pair), base + [strided], field, target, tw_kept, kept_out)
    second = call(slope_second_kernel, one, base, both_p, *slope_tables)
    sent, state = call(slope_kernel, (half_blocks, one), base, device, move(sent), *spectral_tables)
    sent, first = call(nonlinear_kernel, (kept_blocks, one), base, move(sent), second, tw_kept, kept_in, kept_out)
    sent = call(next_kernel, blocks, base, device, move(sent), state, forcing_p, *spectral_tables, mirror)
    sent, next_field = call(
        residual_kernel, (longer, plain), base + [strided, total],
        move(sent), both_p, tw_natural, backward, forward,
    )
    sent, full, coef, sums = call(
        misfit_kernel, (half_blocks, pair, one, shape(8, 2 * rows)), base,
        device, move(sent), tw_natural, forward, tw_natural, backward, mirror,
    )
    sent, product = call(
        joint_kernel, (kept_blocks, one), base, move(sent), first, second, tw_kept, kept_in, kept_out
    )
    second_part = call(slope_second_kernel, one, base, product, *slope_tables)
    sent = call(total_kernel, half_blocks, base, device, move(sent), coef, *spectral_tables)
    field_grad = call(last_kernel, plain, base + [strided], move(sent), second_part, tw_kept, kept_in)
    return next_field, sums[0, 0], field_grad, full


def per_device(devices, initial_field, target_field, forcing):
    members, rows, length = initial_field.shape
    device = lax.axis_index(axes).astype(jnp.int32).reshape(1)
    outer, inner = split_length(length)
    vmem = pl.BlockSpec(memory_space=pltpu.VMEM)
    strided = pltpu.VMEM((length, TILE), jnp.float32)

    def reorder(body, shape, operand):
        return pl.pallas_call(
            functools.partial(body, length, rows),
            out_shape=jax.ShapeDtypeStruct(shape, jnp.float32),
            in_specs=[vmem],
            out_specs=vmem,
            scratch_shapes=[strided],
        )(operand)

    forcing_p = reorder(spread_kernel, (outer, 2 * rows, inner), forcing)
    results = [
        member_step(device, initial_field[m], target_field[m], forcing_p, devices, rows, length)
        for m in range(members)
    ]
    next_field = jnp.stack([one[0] for one in results])
    objective = sum(one[1] for one in results) / (members * length * length)
    field_grad = jnp.stack([one[2] for one in results])
    forcing_grad = reorder(collect_kernel, (2, rows, length), sum(one[3] for one in results))
    return (next_field, objective, field_grad, forcing_grad)


def solution(mesh):
    devices = mesh.shape["px"] * mesh.shape["py"]
    spec = P(None, axes, None)
    return jax.shard_map(
        functools.partial(per_device, devices),
        mesh=mesh,
        in_specs=(spec, spec, spec),
        out_specs=(spec, P(), spec, spec),
        check_vma=False,
    )
```
